32 devices in a mesh: seq: 2 (over core), ctx: 16 (over z, y, x).
Axes of the slice: x: 2, y: 2, z: 4, core: 2. Of those that a mesh axis runs over, the one named last changes fastest.
Arguments:
- hidden: bfloat16 [32768, 7168], P(('seq', 'ctx')), may hold values from -6 to 6
- router_weight: bfloat16 [7168, 256], replicated, may hold values from -0.0625 to 0.0625
- expert_index: int32 [32768, 8], P(('seq', 'ctx')), may hold values from 0 to 255, all different within a row
- lengths: int32 [2], P('seq'), may hold values from 8192 to 16384
Outputs:
- router_grad: float32 [7168, 256], P('ctx')
- balance: float32 [2], P('seq')
The draws below stay inside these ranges and needn't reach their ends.
Inputs may be any that keep to these rules, and one draw needn't show every extreme that they name: A sequence's valid tokens are its first lengths[s] slots, the rest are padding. `expert_index`: each row names 8 different experts.
All inputs are finite; a program needn't handle non-finite values.
Results may differ from the reference program's by a relative error of at most 0.0003.
Values sent between devices are 32-bit elements; how exact they have to be, the bound alone decides.
A program may use at most 128 MiB of HBM per device.

```python
import jax
import jax.numpy as jnp
from jax import lax

D = 7168
E = 256
TOPK = 8
LEN = 16384
SEQS = 2
TOKENS = 32768


def strengthened(values, rng, source, target, parts, factor):
    def block_of(axis_at):
        return (jnp.arange(values.shape[axis_at]) // (values.shape[axis_at] // parts)).reshape((-1,) + (1,) * (values.ndim - 1 - axis_at))

    near = jax.random.permutation(rng, parts)[block_of(target)]
    other_side = (block_of(target) + parts // 2) % parts
    return jnp.where((block_of(source) == near) | (block_of(source) == other_side), factor * values, values)


def level_of(rng, shape, shards, low, largest):
    level = 1.0
    for dim, parts in shards:
        heights = jax.random.uniform(jax.random.fold_in(jax.random.fold_in(rng, 6), dim), (parts,), jnp.float32, low / len(shards), largest / len(shards))
        level = level * jnp.repeat(jnp.exp(heights), shape[dim] // parts).reshape((-1,) + (1,) * (len(shape) - 1 - dim))
    return level


def different_ones(rng, rows, amount, top, lift):
    sequence = jax.random.permutation(jax.random.fold_in(rng, 1), amount)
    boost = sequence
    for power in range(3):
        boost = boost * boost // amount
    boost = boost * lift // amount
    chance = jax.random.randint(jax.random.fold_in(rng, 2), (rows, amount), 0, 4096) + boost
    sure = jax.random.permutation(jax.random.fold_in(rng, 3), rows)[jnp.arange(amount) % rows]
    chance = jnp.where(jnp.arange(rows)[:, None] == sure[None, :], 1 << 14, chance)
    priority = chance * amount + jnp.arange(amount)
    return lax.top_k(priority.astype(jnp.int32), top)[1].astype(jnp.int32)


def bell_draw(rng, extent, width, reach, split=(), kind=jnp.bfloat16):
    gain = level_of(rng, extent, split, -0.22, 0.18) if split else 1.0
    entries = jax.random.normal(rng, extent, jnp.float32) * width * gain
    return jnp.minimum(jnp.maximum(entries, -reach), reach).astype(kind)


def noise_with(key, dims, spread, most, cuts, heavy, kind=jnp.bfloat16):
    result = spread * jax.random.normal(key, dims, jnp.float32)
    if cuts:
        result = result * level_of(key, dims, cuts, -0.22, 0.18)
    return jnp.clip(strengthened(result, jax.random.fold_in(key, 3), *heavy), -most, most).astype(kind)


def setup_inputs(seed: int = 0) -> dict:
    keys = jax.random.split(jax.random.key(seed), 5)
    hidden = noise_with(keys[0], (TOKENS, D), 1.0, 6.0, ((0, 32),), (0, 1, 32, 2.75))
    router_weight = bell_draw(keys[1], (D, E), D ** -0.5, 0.0625)
    expert_index = different_ones(keys[2], TOKENS, E, TOPK, 256)
    lengths = jax.random.randint(keys[3], (SEQS,), LEN // 2, LEN + 1).astype(jnp.int32)
    return {"hidden": hidden, "router_weight": router_weight, "expert_index": expert_index, "lengths": lengths}


loss_scale = 65536.0


def reference(hidden, router_weight, expert_index, lengths):
    hidden_all = hidden.reshape(SEQS, LEN, D)
    index_all = expert_index.reshape(SEQS, LEN, TOPK)

    def one_sequence(packed):
        hidden_seq, index_seq, length_seq = packed
        tokens_live = length_seq.astype(jnp.float32)
        logits = jnp.dot(hidden_seq, router_weight, preferred_element_type=jnp.float32)
        scores = jax.nn.sigmoid(logits)
        row_total = jnp.sum(scores, axis=1, keepdims=True)
        share_of = scores / row_total
        positions = jnp.arange(LEN, dtype=jnp.int32)
        valid_mask = (positions < length_seq.astype(jnp.int32)).astype(jnp.float32)
        expert_ids = jnp.arange(E, dtype=jnp.int32)
        expert_hits = jnp.sum((index_seq[:, :, None] == expert_ids).astype(jnp.float32), axis=1)
        counts = jnp.sum(valid_mask[:, None] * expert_hits, axis=0)
        score_sum = jnp.sum(valid_mask[:, None] * share_of, axis=0)
        fraction = E * counts / (TOPK * tokens_live)
        mean_score = score_sum / tokens_live
        balance = jnp.sum(fraction * mean_score)
        weights = loss_scale * fraction / tokens_live
        weighted = jnp.sum(weights * share_of, axis=1, keepdims=True)
        grad_logits = (weights - weighted) / row_total * scores * (1.0 - scores) * valid_mask[:, None]
        grad_seq = lax.dot_general(hidden_seq.astype(jnp.float32), grad_logits, (((0,), (0,)), ((), ())), precision=lax.Precision.HIGHEST, preferred_element_type=jnp.float32)
        return balance, grad_seq

    balance, grad_stack = lax.map(one_sequence, (hidden_all, index_all, lengths))
    return jnp.sum(grad_stack, axis=0), balance
```

```python
import functools

import jax
import jax.numpy as jnp
from jax import lax
from jax.experimental import pallas as pl
from jax.experimental.pallas import tpu as pltpu
from jax.sharding import PartitionSpec as P

E = 256
TOPK = 8


loss_scale = 65536.0


def shards(hidden, router_weight, expert_index, lengths):
    tok_rows = hidden.shape[0]
    width = hidden.shape[1]
    length_here = lengths[0]
    tokens_live = length_here.astype(jnp.float32)
    positions = lax.axis_index("ctx") * tok_rows + jnp.arange(tok_rows, dtype=jnp.int32)
    valid_mask = (positions < length_here).astype(jnp.float32)
    expert_ids = jnp.arange(E, dtype=jnp.int32)
    expert_hits = jnp.sum((expert_index[:, :, None] == expert_ids).astype(jnp.float32), axis=1)
    counts_local = jnp.sum(valid_mask[:, None] * expert_hits, axis=0)
    logits = jnp.dot(hidden, router_weight, preferred_element_type=jnp.float32)
    scores = jax.nn.sigmoid(logits)
    row_total = jnp.sum(scores, axis=1, keepdims=True)
    share_of = scores / row_total
    score_local = jnp.sum(valid_mask[:, None] * share_of, axis=0)
    counts_all, score_all = lax.psum((counts_local, score_local), "ctx")
    fraction = E * counts_all / (TOPK * tokens_live)
    mean_score = score_all / tokens_live
    balance = jnp.sum(fraction * mean_score).reshape(1)
    weights = loss_scale * fraction / tokens_live
    weighted = jnp.sum(weights * share_of, axis=1, keepdims=True)
    grad_logits = (weights - weighted) / row_total * scores * (1.0 - scores) * valid_mask[:, None]
    seq_count = lax.axis_size("seq")
    ctx_count = lax.axis_size("ctx")
    block_rows = width // (seq_count * ctx_count)
    reordered = hidden.reshape(tok_rows, ctx_count, seq_count, block_rows)
    reordered = jnp.transpose(reordered, (0, 2, 1, 3)).reshape(tok_rows, width)
    columns = reordered.astype(jnp.float32)
    block_sum = lax.psum_scatter(
        lax.dot_general(
            columns,
            grad_logits,
            (((0,), (0,)), ((), ())),
            precision=lax.Precision.HIGHEST,
            preferred_element_type=jnp.float32,
        ),
        ("seq", "ctx"),
        scatter_dimension=0,
        tiled=True,
    )
    router_grad = lax.all_gather(block_sum, "seq", axis=0, tiled=True)
    return (router_grad, balance)


MESH = pl.DeviceIdType.MESH
F32 = jnp.float32
CHUNKS = 2


def remote(src, dst, send, recv, device):
    return pltpu.make_async_remote_copy(
        src_ref=src, dst_ref=dst, send_sem=send, recv_sem=recv, device_id=device, device_id_type=MESH
    )


def kernel(
    n, hid_ref, w_ref, idx_hbm, len_ref, out_ref, bal_ref,
    idx_ref, hid, w, sc, gcat, acc, s, fin, cnt, cnt_all, sco, sco_all,
    ra1, ra2, raz, rbz, rb3, rb4,
    in_sem, cs_s, cs_r, ss_s, ss_r, d_s, d_r, ap_s, ap_r, aq_s, aq_r, az_s, az_r, bz_s, bz_r, bp_s, bp_r, f_s, f_r,
):
    c = lax.axis_index("seq")
    me = lax.axis_index("ctx")
    x, y, z = me % 2, (me // 2) % 2, me // 4
    sp, sq = 1 + c, 2 - c
    p = x + c * (y - x)
    q = y + c * (x - y)
    here = p * sp + q * sq
    p_dev = (c, z * 4 + (1 - p) * sp + q * sq)
    q_dev = (c, z * 4 + p * sp + (1 - q) * sq)
    mate_z, across_z = z + 1 - 2 * (z % 2), 3 - z
    zs = [3 * (1 - z // 2), 2 - z // 2, mate_z, z]
    mate = (c, mate_z * 4 + here)
    across = (c, across_z * 4 + here)
    outer = (z == 0) | (z == 3)
    inner = (z == 1) | (z == 2)
    twin = (1 - c, me)

    tok, width = hid.shape
    rows = tok // CHUNKS
    block = width // n
    half = block // 2
    qb = half * 4 // 14
    qa = half - qb

    idx_copy = pltpu.make_async_copy(idx_hbm, idx_ref, in_sem.at[CHUNKS + 1])
    idx_copy.start()
    w_copy = pltpu.make_async_copy(w_ref, w, in_sem.at[CHUNKS])
    w_copy.start()

    def hid_copy(i):
        span = pl.ds(pl.multiple_of(i * rows, rows), rows)
        return pltpu.make_async_copy(hid_ref.at[span], hid.at[span], in_sem.at[i])

    for i in range(CHUNKS):
        hid_copy(i).start()

    barrier = pltpu.get_barrier_semaphore()

    @pl.loop(1, n)
    def _(d):
        pl.semaphore_signal(barrier, inc=1, device_id=(c, (me + d) % n), device_id_type=MESH)

    pl.semaphore_signal(barrier, inc=1, device_id=twin, device_id_type=MESH)

    length_here = len_ref[0]
    live = jnp.full((1, E), length_here, jnp.int32).astype(F32)

    def valid_of(i):
        at = me * tok + i * rows + lax.broadcasted_iota(jnp.int32, (rows, 1), 0)
        return (at < length_here).astype(F32)

    def count_step(i, total):
        span = pl.ds(pl.multiple_of(i * rows, rows), rows)
        ids = lax.broadcasted_iota(jnp.int32, (E, rows), 0)
        named = idx_ref[:, span]
        hits = jnp.zeros((E, rows), F32)
        for k in range(TOPK):
            hits = hits + (named[k : k + 1, :] == ids).astype(F32)
        at = me * tok + i * rows + lax.broadcasted_iota(jnp.int32, (8, rows), 1)
        valid = (at < length_here).astype(F32).astype(jnp.bfloat16)
        return total + lax.dot_general(
            valid, hits.astype(jnp.bfloat16), (((1,), (1,)), ((), ())), preferred_element_type=F32
        )

    idx_copy.wait()
    counts = lax.fori_loop(0, CHUNKS, count_step, jnp.zeros((8, E), F32))[:1]
    cnt[...] = counts
    cnt_all[me] = counts
    pl.semaphore_wait(barrier, n)

    def stat_copy(d, src, everyone, send, recv):
        return remote(src, everyone.at[me], send.at[d], recv.at[d], (c, (me + d) % n))

    @pl.loop(1, n)
    def _(d):
        stat_copy(d, cnt, cnt_all, cs_s, cs_r).start()

    w_copy.wait()

    def logit_step(i, total):
        span = pl.ds(pl.multiple_of(i * rows, rows), rows)
        hid_copy(i).wait()
        logits = jnp.dot(hid[span, :], w[...], preferred_element_type=F32)
        scores = jax.nn.sigmoid(logits)
        sc[span, :] = scores
        share = scores / jnp.sum(scores, axis=1, keepdims=True)
        return total + jnp.sum(share * valid_of(i), axis=0, keepdims=True)

    score_local = lax.fori_loop(0, CHUNKS, logit_step, jnp.zeros((1, E), F32))
    sco[...] = score_local
    sco_all[me] = score_local

    @pl.loop(1, n)
    def _(d):
        stat_copy(d, cnt, cnt_all, cs_s, cs_r).wait_recv()

    fraction = E * jnp.sum(cnt_all[...], axis=0) / (TOPK * live)
    weights = loss_scale * fraction / live

    @pl.loop(0, CHUNKS)
    def _(i):
        span = pl.ds(pl.multiple_of(i * rows, rows), rows)
        scores = sc[span, :]
        row_total = jnp.sum(scores, axis=1, keepdims=True)
        weighted = jnp.sum(weights * (scores / row_total), axis=1, keepdims=True)
        grad = (weights - weighted) / row_total * scores * (1.0 - scores) * valid_of(i)
        top = grad.astype(jnp.bfloat16)
        gcat[span, :E] = top
        gcat[span, E:] = (grad - top.astype(F32)).astype(jnp.bfloat16)

    @pl.loop(1, n)
    def _(d):
        stat_copy(d, sco, sco_all, ss_s, ss_r).start()

    def pair_send(k, j):
        pair = pl.ds(zs[k] * 4 + 2 * j, 2)
        return remote(acc.at[1 - c, pair], s.at[pair], d_s.at[2 * k + j], d_r.at[2 * k + j], twin)

    def slab_compute(k):
        @pl.loop(0, 2)
        def _(j):
            b = zs[k] * 4 + 2 * j
            columns = pl.ds(pl.multiple_of(b * block, 2 * block), 2 * block)
            both = lax.dot_general(
                hid[:, columns], gcat[...], (((0,), (0,)), ((), ())), preferred_element_type=F32
            )
            part = both[:, :E] + both[:, E:]
            for u in range(2):
                for h in range(2):
                    acc[h, b + u] = part[u * block + h * half : u * block + (h + 1) * half]
            pair_send(k, j).start()

    def slab_join(k):
        for j in range(2):
            pair_send(k, j).wait_recv()

        @pl.loop(0, 4)
        def _(j):
            s[zs[k] * 4 + j] += acc[c, zs[k] * 4 + j]

    lo, hi = pl.ds(0, qa), pl.ds(qa, qb)

    def a_p(k, t):
        return remote(s.at[zs[k] * 4 + (1 - p) * sp + t * sq, lo], ra1.at[k, t], ap_s.at[2 * k + t], ap_r.at[2 * k + t], p_dev)

    def a_q(k):
        return remote(s.at[zs[k] * 4 + p * sp + (1 - q) * sq, lo], ra2.at[k], aq_s.at[k], aq_r.at[k], q_dev)

    def a_at(k):
        return s.at[zs[k] * 4 + here, lo]

    def b_at(k):
        return s.at[pl.ds(zs[k] * 4, 4), hi]

    def line(at, got, send, recv):
        to = [mate, mate, mate, across, across, mate]
        of = [0, 1, 2, 0, 1, 2]
        return [lambda i=i: remote(at(of[i]), got.at[i], send.at[i], recv.at[i], to[i]) for i in range(6)]

    a_z = line(a_at, raz, az_s, az_r)
    b_z = line(b_at, rbz, bz_s, bz_r)

    def outer_send(copies, k):
        @pl.when(outer)
        def _():
            copies[k]().start()

    def inner_pass(copies, at, got, slot, k, out):
        @pl.when(inner)
        def _():
            copies[slot]().wait_recv()
            at(k)[...] += got[slot]
            copies[out]().start()

    def line_end(copies):
        @pl.when(outer)
        def _():
            copies[5]().wait_recv()

        @pl.when(inner)
        def _():
            copies[2]().wait_recv()
            copies[4]().wait_recv()

    def line_sent(copies):
        @pl.when(outer)
        def _():
            for i in range(3):
                copies[i]().wait_send()

        @pl.when(inner)
        def _():
            for i in range(3, 6):
                copies[i]().wait_send()

    def b_p(t):
        return remote(s.at[z * 4 + (1 - p) * sp + t * sq, hi], rb3.at[t], bp_s.at[t], bp_r.at[t], p_dev)

    b_q = remote(s.at[z * 4 + p * sp + (1 - q) * sq, hi], rb4, bp_s.at[2], bp_r.at[2], q_dev)

    def slab_send(k):
        slab_join(k)
        if k < 3:
            outer_send(b_z, k)
        for t in range(2):
            a_p(k, t).start()

    def a_turn(k):
        for t in range(2):
            a_p(k, t).wait_recv()
            s[zs[k] * 4 + p * sp + t * sq, lo] += ra1[k, t]
        a_q(k).start()

    def a_join(k):
        a_q(k).wait_recv()
        a_at(k)[...] += ra2[k]

    for k in range(4):
        slab_compute(k)
        if k > 0:
            slab_send(k - 1)
    inner_pass(b_z, b_at, rbz, 0, 0, 3)
    slab_send(3)
    a_turn(0)
    inner_pass(b_z, b_at, rbz, 1, 1, 4)
    a_turn(1)
    a_join(0)
    outer_send(a_z, 0)
    inner_pass(b_z, b_at, rbz, 3, 2, 5)
    a_turn(2)
    a_join(1)
    outer_send(a_z, 1)
    inner_pass(a_z, a_at, raz, 0, 0, 3)
    a_turn(3)
    line_end(b_z)

    @pl.when(outer)
    def _():
        b_at(3)[...] += rbz[5]

    @pl.when(inner)
    def _():
        b_at(3)[...] += rbz[2] + rbz[4]

    for t in range(2):
        b_p(t).start()
    a_join(2)
    outer_send(a_z, 2)
    inner_pass(a_z, a_at, raz, 1, 1, 4)
    for t in range(2):
        b_p(t).wait_recv()
        s[z * 4 + p * sp + t * sq, hi] += rb3[t]
    b_q.start()
    inner_pass(a_z, a_at, raz, 3, 2, 5)

    @pl.loop(1, n)
    def _(d):
        stat_copy(d, sco, sco_all, ss_s, ss_r).wait_recv()

    mean_score = jnp.sum(sco_all[...], axis=0) / live
    bal_ref[...] = jnp.broadcast_to(jnp.sum(fraction * mean_score, axis=1, keepdims=True), bal_ref.shape)

    b_q.wait_recv()
    fin[c, hi] = s[z * 4 + here, hi] + rb4[...]
    fin_b = remote(fin.at[c, hi], fin.at[c, hi], f_s.at[1], f_r.at[1], twin)
    fin_b.start()
    a_join(3)
    line_end(a_z)

    @pl.when(outer)
    def _():
        fin[c, lo] = s[z * 4 + here, lo] + raz[5]

    @pl.when(inner)
    def _():
        fin[c, lo] = s[z * 4 + here, lo] + raz[2] + raz[4]

    fin_a = remote(fin.at[c, lo], fin.at[c, lo], f_s.at[0], f_r.at[0], twin)
    fin_a.start()
    fin_b.wait_recv()
    fin_a.wait_recv()
    out_ref[pl.ds(0, half), :] = fin[0]
    out_ref[pl.ds(half, half), :] = fin[1]

    @pl.loop(1, n)
    def _(d):
        stat_copy(d, cnt, cnt_all, cs_s, cs_r).wait_send()
        stat_copy(d, sco, sco_all, ss_s, ss_r).wait_send()

    for k in range(4):
        for j in range(2):
            pair_send(k, j).wait_send()
            a_p(k, j).wait_send()
        a_q(k).wait_send()
    line_sent(a_z)
    line_sent(b_z)
    for t in range(2):
        b_p(t).wait_send()
    b_q.wait_send()
    fin_a.wait_send()
    fin_b.wait_send()


def fused(hidden, router_weight, expert_index, lengths):
    n = lax.axis_size("ctx")
    tok, width = hidden.shape
    block = width // n
    half = block // 2
    qb = half * 4 // 14
    qa = half - qb
    dma = pltpu.SemaphoreType.DMA
    bf16 = jnp.bfloat16
    vm = pltpu.VMEM
    grad, bal = pl.pallas_call(
        functools.partial(kernel, n),
        out_shape=(pltpu.VMEM((block, E), F32), pltpu.VMEM((1, 128), F32)),
        in_specs=[
            pl.BlockSpec(memory_space=pltpu.HBM),
            pl.BlockSpec(memory_space=pltpu.HBM),
            pl.BlockSpec(memory_space=pltpu.HBM),
            pl.BlockSpec(memory_space=pltpu.SMEM),
        ],
        out_specs=(pl.BlockSpec(memory_space=pltpu.VMEM), pl.BlockSpec(memory_space=pltpu.VMEM)),
        scratch_shapes=[
            vm((TOPK, tok), jnp.int32), vm((tok, width), bf16), vm((width, E), bf16), vm((tok, E), F32), vm((tok, 2 * E), bf16),
            vm((2, n, half, E), F32), vm((n, half, E), F32), vm((2, half, E), F32),
            vm((1, E), F32), vm((n, 1, E), F32), vm((1, E), F32), vm((n, 1, E), F32),
            vm((4, 2, qa, E), F32), vm((4, qa, E), F32), vm((6, qa, E), F32), vm((6, 4, qb, E), F32),
            vm((2, qb, E), F32), vm((qb, E), F32),
            dma((CHUNKS + 2,)), dma((n,)), dma((n,)), dma((n,)), dma((n,)), dma((8,)), dma((8,)),
            dma((8,)), dma((8,)), dma((4,)), dma((4,)), dma((6,)), dma((6,)), dma((6,)), dma((6,)),
            dma((3,)), dma((3,)), dma((2,)), dma((2,)),
        ],
        compiler_params=pltpu.CompilerParams(
            collective_id=0, has_side_effects=True, vmem_limit_bytes=62914560
        ),
    )(hidden, router_weight, expert_index.T, lengths)
    return grad, bal[0, :1]


def solution(mesh):
    local = fused if (mesh.shape["seq"], mesh.shape["ctx"]) == (2, 16) else shards
    return jax.shard_map(
        local,
        mesh=mesh,
        in_specs=(P(("seq", "ctx"), None), P(), P(("seq", "ctx"), None), P("seq")),
        out_specs=(P("ctx", None), P("seq")),
        check_vma=False,
    )
```

```python
import functools

import jax
import jax.numpy as jnp
from jax import lax
from jax.experimental import pallas as pl
from jax.experimental.pallas import tpu as pltpu
from jax.sharding import PartitionSpec as P

E = 256
TOPK = 8


loss_scale = 65536.0


def shards(hidden, router_weight, expert_index, lengths):
    tok_rows = hidden.shape[0]
    width = hidden.shape[1]
    length_here = lengths[0]
    tokens_live = length_here.astype(jnp.float32)
    positions = lax.axis_index("ctx") * tok_rows + jnp.arange(tok_rows, dtype=jnp.int32)
    valid_mask = (positions < length_here).astype(jnp.float32)
    expert_ids = jnp.arange(E, dtype=jnp.int32)
    expert_hits = jnp.sum((expert_index[:, :, None] == expert_ids).astype(jnp.float32), axis=1)
    counts_local = jnp.sum(valid_mask[:, None] * expert_hits, axis=0)
    logits = jnp.dot(hidden, router_weight, preferred_element_type=jnp.float32)
    scores = jax.nn.sigmoid(logits)
    row_total = jnp.sum(scores, axis=1, keepdims=True)
    share_of = scores / row_total
    score_local = jnp.sum(valid_mask[:, None] * share_of, axis=0)
    counts_all, score_all = lax.psum((counts_local, score_local), "ctx")
    fraction = E * counts_all / (TOPK * tokens_live)
    mean_score = score_all / tokens_live
    balance = jnp.sum(fraction * mean_score).reshape(1)
    weights = loss_scale * fraction / tokens_live
    weighted = jnp.sum(weights * share_of, axis=1, keepdims=True)
    grad_logits = (weights - weighted) / row_total * scores * (1.0 - scores) * valid_mask[:, None]
    seq_count = lax.axis_size("seq")
    ctx_count = lax.axis_size("ctx")
    block_rows = width // (seq_count * ctx_count)
    reordered = hidden.reshape(tok_rows, ctx_count, seq_count, block_rows)
    reordered = jnp.transpose(reordered, (0, 2, 1, 3)).reshape(tok_rows, width)
    columns = reordered.astype(jnp.float32)
    block_sum = lax.psum_scatter(
        lax.dot_general(
            columns,
            grad_logits,
            (((0,), (0,)), ((), ())),
            precision=lax.Precision.HIGHEST,
            preferred_element_type=jnp.float32,
        ),
        ("seq", "ctx"),
        scatter_dimension=0,
        tiled=True,
    )
    router_grad = lax.all_gather(block_sum, "seq", axis=0, tiled=True)
    return (router_grad, balance)


MESH = pl.DeviceIdType.MESH
F32 = jnp.float32
BF16 = jnp.bfloat16
CHUNKS = 7
PARTS = 2
PLANE = 4
LEVELS = 4


def remote(src, dst, send, recv, device):
    return pltpu.make_async_remote_copy(
        src_ref=src, dst_ref=dst, send_sem=send, recv_sem=recv, device_id=device, device_id_type=MESH
    )


def kernel(
    n, hid_ref, w_ref, idx_ref, len_ref, out_ref, bal_ref,
    idx, hid, w, sh, un, gcat, acc, s, fin,
    cnt, cnt_p, cnt_s, cnt_z, cnt_d, tot, sco, sco_p, sco_s, sco_z,
    ra1, ra2, raz, rbz, rb3,
    up, in_sem, st, d_s, d_r, ap_s, ap_r, aq_s, aq_r, az_s, az_r, bz_s, bz_r, bp_s, bp_r, f_s, f_r,
):
    c = lax.axis_index("seq")
    me = lax.axis_index("ctx")
    x, y, z = me % 2, (me // 2) % 2, me // 4
    sp, sq = 1 + c, 2 - c
    p = x + c * (y - x)
    q = y + c * (x - y)
    here = p * sp + q * sq
    p_dev = (c, z * 4 + (1 - p) * sp + q * sq)
    q_dev = (c, z * 4 + p * sp + (1 - q) * sq)
    mate_z, across_z = z + 1 - 2 * (z % 2), 3 - z
    zs = [3 * (1 - z // 2), 2 - z // 2, mate_z, z]
    mate = (c, mate_z * 4 + here)
    across = (c, across_z * 4 + here)
    outer = (z == 0) | (z == 3)
    inner = (z == 1) | (z == 2)
    twin = (1 - c, me)

    def plane_peer(d):
        return (c, z * 4 + (here + d) % PLANE)

    def line_peer(d):
        return (c, ((z + d) % LEVELS) * 4 + here)

    tok, width = hid.shape
    part_w = width // CHUNKS
    big = tok // PARTS
    block = width // n
    half = block // 2
    qb = half * 3 // 14
    qa = half - qb
    qh = qa // 2

    barrier = pltpu.get_barrier_semaphore()
    for d in range(1, PLANE):
        pl.semaphore_signal(barrier, inc=1, device_id=plane_peer(d), device_id_type=MESH)
    pl.semaphore_signal(barrier, inc=1, device_id=twin, device_id_type=MESH)

    @pl.loop((z + 1) * PLANE, n)
    def _(d):
        pl.semaphore_signal(barrier, inc=1, device_id=(c, d), device_id_type=MESH)

    idx_copy = pltpu.make_async_copy(idx_ref, idx, in_sem.at[2 * CHUNKS])
    idx_copy.start()

    def w_copy(i):
        span = pl.ds(pl.multiple_of(i * part_w, part_w), part_w)
        return pltpu.make_async_copy(w_ref.at[span], w.at[span], in_sem.at[CHUNKS + i])

    def hid_copy(i):
        span = pl.ds(pl.multiple_of(i * part_w, part_w), part_w)
        return pltpu.make_async_copy(hid_ref.at[:, span], hid.at[:, span], in_sem.at[i])

    @pl.loop(0, CHUNKS)
    def _(i):
        w_copy(i).start()
        hid_copy(i).start()

    length_here = len_ref[0]
    live = jnp.full((1, E), length_here, jnp.int32).astype(F32)

    def count_step(i, total):
        span = pl.ds(pl.multiple_of(i * big, big), big)
        ids = lax.broadcasted_iota(jnp.int32, (E, big), 0).astype(BF16)
        named = idx[:, span].astype(F32)
        hits = jnp.zeros((E, big), BF16)
        for k in range(TOPK):
            one = jnp.broadcast_to(named[k : k + 1, :], (E, big)).astype(BF16)
            hits = hits + jnp.where(one == ids, BF16(1), BF16(0))
        at = me * tok + i * big + lax.broadcasted_iota(jnp.int32, (8, big), 1)
        valid = (at < length_here).astype(F32).astype(BF16)
        return total + lax.dot_general(
            valid, hits, (((1,), (1,)), ((), ())), preferred_element_type=F32
        )

    def plane_copy(d, src, everyone, base):
        return remote(src, everyone.at[here], st.at[base], st.at[base + 1], plane_peer(d))

    def line_copy(d, src, everyone, base):
        return remote(src, everyone.at[z], st.at[base + 2], st.at[base + 3], line_peer(d))

    def down_copy(d):
        slot = (z - d // PLANE - 1) * PLANE + here
        return remote(cnt, cnt_d.at[slot], st.at[8], st.at[9], (c, d))

    def up_copy(d):
        return remote(cnt_s, cnt_z.at[z], st.at[2], st.at[3], (c, d * PLANE + here))

    def sent(ref, sem):
        remote(ref, ref, sem, sem, twin).wait_send()

    def came(ref, sem):
        remote(ref, ref, sem, sem, twin).wait_recv()

    def plane_send(value, src, everyone, base):
        src[...] = value
        everyone[here] = value
        for d in range(1, PLANE):
            plane_copy(d, src, everyone, base).start()

    def plane_total(everyone, base):
        came(everyone.at[pl.ds(0, PLANE - 1)], st.at[base + 1])
        return jnp.sum(everyone[...], axis=0)
    idx_copy.wait()
    counts = lax.fori_loop(0, PARTS, count_step, jnp.zeros((8, E), F32))[:1]
    pl.semaphore_wait(barrier, PLANE * (z + 1))

    @pl.loop(0, z)
    def _(d):
        pl.semaphore_signal(up, inc=1, device_id=(c, d * PLANE + here), device_id_type=MESH)
    plane_send(counts, cnt, cnt_p, 0)

    @pl.loop(0, z * PLANE)
    def _(d):
        down_copy(d).start()

    sh[...] = jnp.zeros_like(sh)
    turn = 5 - (x + y + 1) // 2

    def logit_step(i):
        @pl.when(i == turn)
        def _():
            total = plane_total(cnt_p, 0)
            cnt_s[...] = total
            tot[...] = total

            @pl.when(z < LEVELS - 1)
            def _():
                pl.semaphore_wait(up, LEVELS - 1 - z)

            @pl.loop(z + 1, LEVELS)
            def _(d):
                up_copy(d).start()

        span = pl.ds(pl.multiple_of(i * part_w, part_w), part_w)
        w_copy(i).wait()
        hid_copy(i).wait()
        sh[...] += jnp.dot(hid[:, span], w[span, :], preferred_element_type=F32)

    pl.loop(0, CHUNKS)(logit_step)

    def score_step(i, total):
        span = pl.ds(pl.multiple_of(i * big, big), big)
        scores = jax.nn.sigmoid(sh[span, :])
        at = me * tok + i * big + lax.broadcasted_iota(jnp.int32, (big, 1), 0)
        valid = (at < length_here).astype(F32)
        share = scores / jnp.sum(scores, axis=1, keepdims=True)
        live_share = share * valid
        sh[span, :] = share
        un[span, :] = live_share * (1.0 - scores)
        return total + jnp.sum(live_share, axis=0, keepdims=True)

    score_local = lax.fori_loop(0, PARTS, score_step, jnp.zeros((1, E), F32))
    for k in range(LEVELS):
        @pl.when(z == k)
        def _():
            total = tot[...]
            if k < LEVELS - 1:
                far = pl.ds(0, PLANE * (LEVELS - 1 - k))
                came(cnt_d.at[far], st.at[9])
                total = total + jnp.sum(cnt_d[far], axis=0)
            if k > 0:
                near = pl.ds(0, k)
                came(cnt_z.at[near], st.at[3])
                total = total + jnp.sum(cnt_z[near], axis=0)
            tot[...] = total

    fraction = E * tot[...] / (TOPK * live)
    weights = loss_scale * fraction / live

    @pl.loop(0, PARTS)
    def _(i):
        span = pl.ds(pl.multiple_of(i * big, big), big)
        weighted = jnp.sum(weights * sh[span, :], axis=1, keepdims=True)
        grad = (weights - weighted) * un[span, :]
        top = grad.astype(BF16)
        gcat[span, :E] = top
        gcat[span, E:] = (grad - top.astype(F32)).astype(BF16)

    plane_send(score_local, sco, sco_p, 4)

    def level(k):
        return jnp.where(k == 0, zs[0], jnp.where(k == 1, zs[1], jnp.where(k == 2, zs[2], zs[3])))

    def pair_at(k, j):
        row = (1 - y) + j * (2 * y - 1)
        zk = zs[k] if isinstance(k, int) else level(k)
        return zk * 4 + 2 * row

    def pair_send(i):
        pair = pl.ds(pair_at(i // 2, i % 2), 2)
        return remote(acc.at[1 - c, pair], s.at[pair], d_s.at[0], d_r.at[i], twin)

    lo, hi = pl.ds(0, qa), pl.ds(qa, qb)

    def side(o):
        return (1 - q) + o * (2 * q - 1)

    def a_p(k, o):
        zk = zs[k] if isinstance(k, int) else level(k)
        return remote(
            s.at[zk * 4 + (1 - p) * sp + side(o) * sq, lo], ra1.at[k, o], ap_s.at[0], ap_r.at[2 * k + o], p_dev
        )

    def a_q(k):
        return remote(s.at[zs[k] * 4 + p * sp + (1 - q) * sq, lo], ra2.at[k], aq_s.at[0], aq_r.at[k], q_dev)

    def a_at(k, h):
        return s.at[zs[k] * 4 + here, pl.ds(h * qh, qh)]

    def b_at(k, j):
        return s.at[pl.ds(pair_at(k, j), 2), hi]

    TO = [mate, mate, mate, across, across, mate]
    OF = [0, 1, 2, 0, 1, 2]
    AT = [0, 1, 3, 2, 4, 5]

    def a_z(i, h):
        return remote(a_at(OF[i], h), raz.at[h, AT[i]], az_s.at[0], az_r.at[min(2 * AT[i], 6) + h], TO[i])

    def b_z(i, h):
        return remote(b_at(OF[i], h), rbz.at[AT[i], h], bz_s.at[0], bz_r.at[2 * AT[i] + h if AT[i] < 3 else 6], TO[i])

    def b_z_out(k, j):
        pair = pl.ds(pair_at(k, j), 2)
        slot = k + k // 2
        return remote(s.at[pair, hi], rbz.at[slot, j], bz_s.at[0], bz_r.at[jnp.minimum(2 * slot + j, 6)], mate)

    def join(i):
        k, j = i // 2, i % 2
        pair_send(i).wait_recv()
        pair = pl.ds(pair_at(k, j), 2)
        s[pair] += acc[c, pair]

        @pl.when((c == 0) & (k < 3))
        def _():
            a_p(k, j).start()

        @pl.when((c == 1) & (k < 3) & (j == 0))
        def _():
            a_p(k, 0).start()
            a_p(k, 1).start()

        @pl.when(outer & (k < 3))
        def _():
            b_z_out(k, j).start()

    def a_turn(k, o):
        a_p(k, o).wait_recv()
        s[zs[k] * 4 + p * sp + side(o) * sq, lo] += ra1[k, o]
        if o == 0:
            a_q(k).start()

    def a_join(k):
        a_q(k).wait_recv()
        s[zs[k] * 4 + here, lo] += ra2[k]

    def a_out(k):
        @pl.when(outer)
        def _():
            for h in range(2):
                a_z(k, h).start()

    def passing(copies, at, got, slot, k, out, h):
        copies(slot, h).wait_recv()
        at(k, h)[...] += got[h, AT[slot]] if got is raz else got[AT[slot], h]
        copies(out, h).start()

    def b_pass(slot, h):
        k, out = {0: (0, 3), 1: (1, 4), 3: (2, 5)}[slot]

        @pl.when(inner)
        def _():
            passing(b_z, b_at, rbz, slot, k, out, h)

    def a_pass(slot, h):
        k, out = {0: (0, 3), 1: (1, 4), 3: (2, 5)}[slot]

        @pl.when(inner)
        def _():
            passing(a_z, a_at, raz, slot, k, out, h)

    def b_end():
        @pl.when(outer)
        def _():
            came(rbz.at[5], bz_r.at[6])
            for h in range(2):
                b_at(3, h)[...] += rbz[5, h]

        @pl.when(inner)
        def _():
            came(rbz.at[pl.ds(3, 2)], bz_r.at[6])
            for h in range(2):
                b_at(3, h)[...] += rbz[3, h] + rbz[4, h]

    def b_p(o):
        return remote(s.at[z * 4 + (1 - p) * sp + side(o) * sq, hi], rb3.at[o], bp_s.at[0], bp_r.at[o], p_dev)

    b_q = remote(s.at[z * 4 + p * sp + (1 - q) * sq, hi], rb3.at[2], bp_s.at[0], bp_r.at[2], q_dev)

    def b_turn(o):
        b_p(o).wait_recv()
        s[z * 4 + p * sp + side(o) * sq, hi] += rb3[o]
        if o == 0:
            b_q.start()

    def fin_a(h):
        part = fin.at[c, pl.ds(h * qh, qh)]
        return remote(part, part, f_s.at[0], f_r.at[0], twin)

    fin_b = remote(fin.at[c, hi], fin.at[c, hi], f_s.at[0], f_r.at[0], twin)

    def a_end(h):
        part = pl.ds(h * qh, qh)

        @pl.when(outer)
        def _():
            came(raz.at[h, 5], az_r.at[6 + h])
            fin[c, part] = s[z * 4 + here, part] + raz[h, 5]

        @pl.when(inner)
        def _():
            came(raz.at[h, pl.ds(3, 2)], az_r.at[6 + h])
            fin[c, part] = s[z * 4 + here, part] + raz[h, 3] + raz[h, 4]

        fin_a(h).start()

    @pl.loop(0, 8)
    def _(i):
        b = pair_at(i // 2, i % 2)
        columns = pl.ds(pl.multiple_of(b * block, 2 * block), 2 * block)
        both = lax.dot_general(
            hid[:, columns], gcat[...], (((0,), (0,)), ((), ())), preferred_element_type=F32
        )
        part = both[:, :E] + both[:, E:]
        for u in range(2):
            for h in range(2):
                acc[h, b + u] = part[u * block + h * half : u * block + (h + 1) * half]
        pair_send(i).start()

        @pl.when(i > 0)
        def _():
            join(i - 1)

        @pl.when(i == 4)
        def _():
            a_turn(0, 0)

        @pl.when(i == 5)
        def _():
            b_pass(0, 0)

        @pl.when(i == 6)
        def _():
            a_turn(0, 1)
            b_pass(0, 1)

    join(7)
    total = plane_total(sco_p, 4)
    sco_s[...] = total
    sco_z[z] = total
    for d in range(1, LEVELS):
        line_copy(d, sco_s, sco_z, 4).start()
    b_pass(3, 0)
    b_pass(1, 0)
    a_turn(1, 0)
    a_join(0)
    a_out(0)
    b_pass(3, 1)
    b_pass(1, 1)
    a_turn(1, 1)
    b_end()
    for o in range(2):
        b_p(o).start()
    for o in range(2):
        a_p(3, o).start()
    a_pass(0, 0)
    a_turn(2, 0)
    a_join(1)
    a_out(1)
    a_pass(0, 1)
    b_turn(0)
    a_turn(2, 1)
    b_turn(1)
    came(sco_z.at[pl.ds(0, LEVELS - 1)], st.at[7])
    mean_score = jnp.sum(sco_z[...], axis=0) / live
    bal_ref[...] = jnp.broadcast_to(jnp.sum(fraction * mean_score, axis=1, keepdims=True), bal_ref.shape)
    a_pass(1, 0)
    a_pass(1, 1)
    a_turn(3, 0)
    a_join(2)
    a_out(2)
    a_pass(3, 0)
    a_pass(3, 1)
    b_q.wait_recv()
    fin[c, hi] = s[z * 4 + here, hi] + rb3[2]
    fin_b.start()
    a_turn(3, 1)
    a_join(3)
    a_end(0)
    a_end(1)
    came(fin.at[1 - c], f_r.at[0])
    out_ref[pl.ds(0, half), :] = fin[0]
    out_ref[pl.ds(half, half), :] = fin[1]

    near = pl.ds(0, PLANE - 1)
    sent(cnt_p.at[near], st.at[0])
    sent(sco_p.at[near], st.at[4])
    sent(sco_z.at[near], st.at[6])
    for k in range(LEVELS):
        @pl.when(z == k)
        def _():
            if k < LEVELS - 1:
                sent(cnt_z.at[pl.ds(0, LEVELS - 1 - k)], st.at[2])
            if k > 0:
                sent(cnt_d.at[pl.ds(0, PLANE * k)], st.at[8])

    sent(s, d_s.at[0])
    sent(ra1, ap_s.at[0])
    sent(ra2, aq_s.at[0])
    sent(raz.at[0], az_s.at[0])
    sent(rbz.at[pl.ds(0, 3)], bz_s.at[0])
    sent(rb3, bp_s.at[0])
    sent(fin.at[c], f_s.at[0])


def fused(hidden, router_weight, expert_index, lengths):
    n = lax.axis_size("ctx")
    tok, width = hidden.shape
    block = width // n
    half = block // 2
    qb = half * 3 // 14
    qa = half - qb
    dma = pltpu.SemaphoreType.DMA
    vm = pltpu.VMEM
    grad, bal = pl.pallas_call(
        functools.partial(kernel, n),
        out_shape=(pltpu.VMEM((block, E), F32), pltpu.VMEM((1, 128), F32)),
        in_specs=[
            pl.BlockSpec(memory_space=pltpu.HBM),
            pl.BlockSpec(memory_space=pltpu.HBM),
            pl.BlockSpec(memory_space=pltpu.HBM),
            pl.BlockSpec(memory_space=pltpu.SMEM),
        ],
        out_specs=(pl.BlockSpec(memory_space=pltpu.VMEM), pl.BlockSpec(memory_space=pltpu.VMEM)),
        scratch_shapes=[
            vm((TOPK, tok), jnp.int32), vm((tok, width), BF16), vm((width, E), BF16),
            vm((tok, E), F32), vm((tok, E), F32), vm((tok, 2 * E), BF16),
            vm((2, n, half, E), F32), vm((n, half, E), F32), vm((2, half, E), F32),
            vm((1, E), F32), vm((PLANE, 1, E), F32), vm((1, E), F32), vm((LEVELS, 1, E), F32),
            vm((PLANE * (LEVELS - 1), 1, E), F32), vm((1, E), F32),
            vm((1, E), F32), vm((PLANE, 1, E), F32), vm((1, E), F32), vm((LEVELS, 1, E), F32),
            vm((4, 2, qa, E), F32), vm((4, qa, E), F32), vm((2, 6, qa // 2, E), F32), vm((6, 2, 2, qb, E), F32),
            vm((3, qb, E), F32), pltpu.SemaphoreType.REGULAR,
            dma((2 * CHUNKS + 1,)), dma((10,)), dma((1,)), dma((8,)),
            dma((1,)), dma((8,)), dma((1,)), dma((4,)), dma((1,)), dma((8,)), dma((1,)), dma((7,)),
            dma((1,)), dma((3,)), dma((1,)), dma((1,)),
        ],
        compiler_params=pltpu.CompilerParams(
            collective_id=0, has_side_effects=True, vmem_limit_bytes=62914560
        ),
    )(hidden, router_weight, expert_index.T, lengths)
    return grad, bal[0, :1]


def solution(mesh):
    local = fused if (mesh.shape["seq"], mesh.shape["ctx"]) == (2, 16) else shards
    return jax.shard_map(
        local,
        mesh=mesh,
        in_specs=(P(("seq", "ctx"), None), P(), P(("seq", "ctx"), None), P("seq")),
        out_specs=(P("ctx", None), P("seq")),
        check_vma=False,
    )
```

```python
import functools

import jax
import jax.numpy as jnp
from jax import lax
from jax.experimental import pallas as pl
from jax.experimental.pallas import tpu as pltpu
from jax.sharding import PartitionSpec as P

E = 256
TOPK = 8


loss_scale = 65536.0


def shards(hidden, router_weight, expert_index, lengths):
    tok_rows = hidden.shape[0]
    width = hidden.shape[1]
    length_here = lengths[0]
    tokens_live = length_here.astype(jnp.float32)
    positions = lax.axis_index("ctx") * tok_rows + jnp.arange(tok_rows, dtype=jnp.int32)
    valid_mask = (positions < length_here).astype(jnp.float32)
    expert_ids = jnp.arange(E, dtype=jnp.int32)
    expert_hits = jnp.sum((expert_index[:, :, None] == expert_ids).astype(jnp.float32), axis=1)
    counts_local = jnp.sum(valid_mask[:, None] * expert_hits, axis=0)
    logits = jnp.dot(hidden, router_weight, preferred_element_type=jnp.float32)
    scores = jax.nn.sigmoid(logits)
    row_total = jnp.sum(scores, axis=1, keepdims=True)
    share_of = scores / row_total
    score_local = jnp.sum(valid_mask[:, None] * share_of, axis=0)
    counts_all, score_all = lax.psum((counts_local, score_local), "ctx")
    fraction = E * counts_all / (TOPK * tokens_live)
    mean_score = score_all / tokens_live
    balance = jnp.sum(fraction * mean_score).reshape(1)
    weights = loss_scale * fraction / tokens_live
    weighted = jnp.sum(weights * share_of, axis=1, keepdims=True)
    grad_logits = (weights - weighted) / row_total * scores * (1.0 - scores) * valid_mask[:, None]
    seq_count = lax.axis_size("seq")
    ctx_count = lax.axis_size("ctx")
    block_rows = width // (seq_count * ctx_count)
    reordered = hidden.reshape(tok_rows, ctx_count, seq_count, block_rows)
    reordered = jnp.transpose(reordered, (0, 2, 1, 3)).reshape(tok_rows, width)
    columns = reordered.astype(jnp.float32)
    block_sum = lax.psum_scatter(
        lax.dot_general(
            columns,
            grad_logits,
            (((0,), (0,)), ((), ())),
            precision=lax.Precision.HIGHEST,
            preferred_element_type=jnp.float32,
        ),
        ("seq", "ctx"),
        scatter_dimension=0,
        tiled=True,
    )
    router_grad = lax.all_gather(block_sum, "seq", axis=0, tiled=True)
    return (router_grad, balance)


MESH = pl.DeviceIdType.MESH
F32 = jnp.float32
BF16 = jnp.bfloat16
CHUNKS = 7
PARTS = 2
SMALL = 4
PLANE = 4
LEVELS = 4


def remote(src, dst, send, recv, device):
    return pltpu.make_async_remote_copy(
        src_ref=src, dst_ref=dst, send_sem=send, recv_sem=recv, device_id=device, device_id_type=MESH
    )


def kernel(
    n, hid_ref, w_ref, idx_ref, len_hbm, out_ref, bal_ref,
    len_ref, idx, hid, w, sh, un, gcat, acc, s, fin,
    cnt, cnt_p, cnt_s, cnt_z, cnt_d, tot, sco, sco_p, sco_s, sco_z,
    ra1, ra2, raz, rbz, rb3,
    up, in_sem, st, d_s, d_r, ap_s, ap_r, aq_s, aq_r, az_s, az_r, bz_s, bz_r, bp_s, bp_r, f_s, f_r,
):
    c = lax.axis_index("seq")
    me = lax.axis_index("ctx")
    x, y, z = me % 2, (me // 2) % 2, me // 4
    sp, sq = 1 + c, 2 - c
    p = x + c * (y - x)
    q = y + c * (x - y)
    here = p * sp + q * sq
    p_dev = (c, z * 4 + (1 - p) * sp + q * sq)
    q_dev = (c, z * 4 + p * sp + (1 - q) * sq)
    mate_z, across_z = z + 1 - 2 * (z % 2), 3 - z
    zs = [3 * (1 - z // 2), 2 - z // 2, mate_z, z]
    mate = (c, mate_z * 4 + here)
    across = (c, across_z * 4 + here)
    outer = (z == 0) | (z == 3)
    inner = (z == 1) | (z == 2)
    twin = (1 - c, me)

    def plane_peer(d):
        return (c, z * 4 + (here + d) % PLANE)

    def line_peer(d):
        return (c, ((z + d) % LEVELS) * 4 + here)

    tok, width = hid.shape
    part_w = width // CHUNKS
    big = tok // PARTS
    small = tok // SMALL
    block = width // n
    half = block // 2
    qb = half * 3 // 14
    qa = half - qb
    qh = qa // 2

    len_copy = pltpu.make_async_copy(len_hbm, len_ref, in_sem.at[2 * CHUNKS + 1])
    len_copy.start()
    idx_copy = pltpu.make_async_copy(idx_ref, idx, in_sem.at[2 * CHUNKS])
    idx_copy.start()

    def w_copy(i):
        span = pl.ds(pl.multiple_of(i * part_w, part_w), part_w)
        return pltpu.make_async_copy(w_ref.at[span], w.at[span], in_sem.at[CHUNKS + i])

    def hid_copy(i):
        span = pl.ds(pl.multiple_of(i * part_w, part_w), part_w)
        return pltpu.make_async_copy(hid_ref.at[:, span], hid.at[:, span], in_sem.at[i])

    @pl.loop(0, CHUNKS)
    def _(i):
        w_copy(i).start()
        hid_copy(i).start()


    barrier = pltpu.get_barrier_semaphore()
    for d in range(1, PLANE):
        pl.semaphore_signal(barrier, inc=1, device_id=plane_peer(d), device_id_type=MESH)
    pl.semaphore_signal(barrier, inc=1, device_id=twin, device_id_type=MESH)

    @pl.loop((z + 1) * PLANE, n)
    def _(d):
        pl.semaphore_signal(barrier, inc=1, device_id=(c, d), device_id_type=MESH)

    def count_step(length_here, i, total):
        span = pl.ds(pl.multiple_of(i * big, big), big)
        ids = lax.broadcasted_iota(jnp.int32, (E, big), 0).astype(BF16)
        named = idx[:, span].astype(F32)
        hits = jnp.zeros((E, big), BF16)
        for k in range(TOPK):
            one = jnp.broadcast_to(named[k : k + 1, :], (E, big)).astype(BF16)
            hits = hits + jnp.where(one == ids, BF16(1), BF16(0))
        at = me * tok + i * big + lax.broadcasted_iota(jnp.int32, (8, big), 1)
        valid = (at < length_here).astype(F32).astype(BF16)
        return total + lax.dot_general(
            valid, hits, (((1,), (1,)), ((), ())), preferred_element_type=F32
        )

    def plane_copy(d, src, everyone, base):
        return remote(src, everyone.at[here], st.at[base], st.at[base + 1], plane_peer(d))

    def line_copy(d, src, everyone, base):
        return remote(src, everyone.at[z], st.at[base + 2], st.at[base + 3], line_peer(d))

    def down_copy(d):
        slot = (z - d // PLANE - 1) * PLANE + here
        return remote(cnt, cnt_d.at[slot], st.at[8], st.at[9], (c, d))

    def up_copy(d):
        return remote(cnt_s, cnt_z.at[z], st.at[2], st.at[3], (c, d * PLANE + here))

    def sent(ref, sem):
        remote(ref, ref, sem, sem, twin).wait_send()

    def came(ref, sem):
        remote(ref, ref, sem, sem, twin).wait_recv()

    def plane_send(value, src, everyone, base):
        src[...] = value
        everyone[here] = value
        for d in range(1, PLANE):
            plane_copy(d, src, everyone, base).start()

    def plane_total(everyone, base):
        came(everyone.at[pl.ds(0, PLANE - 1)], st.at[base + 1])
        return jnp.sum(everyone[...], axis=0)
    len_copy.wait()
    idx_copy.wait()
    length_here = len_ref[0]
    live = jnp.full((1, E), length_here, jnp.int32).astype(F32)
    counts = lax.fori_loop(0, PARTS, functools.partial(count_step, length_here), jnp.zeros((8, E), F32))[:1]
    pl.semaphore_wait(barrier, PLANE * (z + 1))

    @pl.loop(0, z)
    def _(d):
        pl.semaphore_signal(up, inc=1, device_id=(c, d * PLANE + here), device_id_type=MESH)
    plane_send(counts, cnt, cnt_p, 0)

    @pl.loop(0, z * PLANE)
    def _(d):
        down_copy(d).start()

    sh[...] = jnp.zeros_like(sh)
    turn = 5 - (x + y + 1) // 2

    def logit_step(i):
        @pl.when(i == turn)
        def _():
            total = plane_total(cnt_p, 0)
            cnt_s[...] = total
            tot[...] = total

            @pl.when(z < LEVELS - 1)
            def _():
                pl.semaphore_wait(up, LEVELS - 1 - z)

            @pl.loop(z + 1, LEVELS)
            def _(d):
                up_copy(d).start()

        span = pl.ds(pl.multiple_of(i * part_w, part_w), part_w)
        w_copy(i).wait()
        hid_copy(i).wait()
        sh[...] += jnp.dot(hid[:, span], w[span, :], preferred_element_type=F32)

    pl.loop(0, CHUNKS - 1)(logit_step)
    w_copy(CHUNKS - 1).wait()
    hid_copy(CHUNKS - 1).wait()
    last = pl.ds((CHUNKS - 1) * part_w, part_w)

    def score_step(i, total):
        span = pl.ds(i * small, small)
        logits = sh[span, :] + jnp.dot(hid[span, last], w[last, :], preferred_element_type=F32)
        scores = jax.nn.sigmoid(logits)
        at = me * tok + i * small + lax.broadcasted_iota(jnp.int32, (small, 1), 0)
        valid = (at < length_here).astype(F32)
        share = scores / jnp.sum(scores, axis=1, keepdims=True)
        live_share = share * valid
        sh[span, :] = share
        un[span, :] = live_share * (1.0 - scores)
        return total + jnp.sum(live_share, axis=0, keepdims=True)

    score_local = jnp.zeros((1, E), F32)
    for i in range(SMALL):
        score_local = score_step(i, score_local)
    for k in range(LEVELS):
        @pl.when(z == k)
        def _():
            total = tot[...]
            if k < LEVELS - 1:
                far = pl.ds(0, PLANE * (LEVELS - 1 - k))
                came(cnt_d.at[far], st.at[9])
                total = total + jnp.sum(cnt_d[far], axis=0)
            if k > 0:
                near = pl.ds(0, k)
                came(cnt_z.at[near], st.at[3])
                total = total + jnp.sum(cnt_z[near], axis=0)
            tot[...] = total

    fraction = E * tot[...] / (TOPK * live)
    weights = loss_scale * fraction / live

    @pl.loop(0, PARTS)
    def _(i):
        span = pl.ds(pl.multiple_of(i * big, big), big)
        weighted = jnp.sum(weights * sh[span, :], axis=1, keepdims=True)
        grad = (weights - weighted) * un[span, :]
        top = grad.astype(BF16)
        gcat[span, :E] = top
        gcat[span, E:] = (grad - top.astype(F32)).astype(BF16)

    plane_send(score_local, sco, sco_p, 4)

    def level(k):
        return jnp.where(k == 0, zs[0], jnp.where(k == 1, zs[1], jnp.where(k == 2, zs[2], zs[3])))

    def pair_at(k, j):
        row = (1 - y) + j * (2 * y - 1)
        zk = zs[k] if isinstance(k, int) else level(k)
        return zk * 4 + 2 * row

    def pair_send(i):
        pair = pl.ds(pair_at(i // 2, i % 2), 2)
        return remote(acc.at[1 - c, pair], s.at[pair], d_s.at[0], d_r.at[i], twin)

    lo, hi = pl.ds(0, qa), pl.ds(qa, qb)

    def side(o):
        return (1 - q) + o * (2 * q - 1)

    def a_p(k, o):
        zk = zs[k] if isinstance(k, int) else level(k)
        return remote(
            s.at[zk * 4 + (1 - p) * sp + side(o) * sq, lo], ra1.at[k, o], ap_s.at[0], ap_r.at[2 * k + o], p_dev
        )

    def a_q(k):
        return remote(s.at[zs[k] * 4 + p * sp + (1 - q) * sq, lo], ra2.at[k], aq_s.at[0], aq_r.at[k], q_dev)

    def a_at(k, h):
        return s.at[zs[k] * 4 + here, pl.ds(h * qh, qh)]

    def b_at(k, j):
        return s.at[pl.ds(pair_at(k, j), 2), hi]

    TO = [mate, mate, mate, across, across, mate]
    OF = [0, 1, 2, 0, 1, 2]
    AT = [0, 1, 3, 2, 4, 5]

    def a_z(i, h):
        return remote(a_at(OF[i], h), raz.at[h, AT[i]], az_s.at[0], az_r.at[min(2 * AT[i], 6) + h], TO[i])

    def b_z(i, h):
        return remote(b_at(OF[i], h), rbz.at[AT[i], h], bz_s.at[0], bz_r.at[2 * AT[i] + h if AT[i] < 3 else 6], TO[i])

    def b_z_out(k, j):
        pair = pl.ds(pair_at(k, j), 2)
        slot = k + k // 2
        return remote(s.at[pair, hi], rbz.at[slot, j], bz_s.at[0], bz_r.at[jnp.minimum(2 * slot + j, 6)], mate)

    def join(i):
        k, j = i // 2, i % 2
        pair_send(i).wait_recv()
        pair = pl.ds(pair_at(k, j), 2)
        s[pair] += acc[c, pair]

        @pl.when((c == 0) & (i < 7))
        def _():
            a_p(k, j).start()

        @pl.when((c == 1) & (j == 0))
        def _():
            a_p(k, 0).start()

        @pl.when((c == 1) & (j == 0) & (k < 3))
        def _():
            a_p(k, 1).start()

        @pl.when(outer & (k < 3))
        def _():
            b_z_out(k, j).start()

    def a_turn(k, o):
        a_p(k, o).wait_recv()
        s[zs[k] * 4 + p * sp + side(o) * sq, lo] += ra1[k, o]
        if o == 0:
            a_q(k).start()

    def a_join(k):
        a_q(k).wait_recv()
        s[zs[k] * 4 + here, lo] += ra2[k]

    def a_out(k):
        @pl.when(outer)
        def _():
            for h in range(2):
                a_z(k, h).start()

    def passing(copies, at, got, slot, k, out, h):
        copies(slot, h).wait_recv()
        at(k, h)[...] += got[h, AT[slot]] if got is raz else got[AT[slot], h]
        copies(out, h).start()

    def b_pass(slot, h):
        k, out = {0: (0, 3), 1: (1, 4), 3: (2, 5)}[slot]

        @pl.when(inner)
        def _():
            passing(b_z, b_at, rbz, slot, k, out, h)

    def a_pass(slot, h):
        k, out = {0: (0, 3), 1: (1, 4), 3: (2, 5)}[slot]

        @pl.when(inner)
        def _():
            passing(a_z, a_at, raz, slot, k, out, h)

    def b_end():
        @pl.when(outer)
        def _():
            came(rbz.at[5], bz_r.at[6])
            for h in range(2):
                b_at(3, h)[...] += rbz[5, h]

        @pl.when(inner)
        def _():
            came(rbz.at[pl.ds(3, 2)], bz_r.at[6])
            for h in range(2):
                b_at(3, h)[...] += rbz[3, h] + rbz[4, h]

    def b_p(o):
        return remote(s.at[z * 4 + (1 - p) * sp + side(o) * sq, hi], rb3.at[o], bp_s.at[0], bp_r.at[o], p_dev)

    b_q = remote(s.at[z * 4 + p * sp + (1 - q) * sq, hi], rb3.at[2], bp_s.at[0], bp_r.at[2], q_dev)

    def b_turn(o):
        b_p(o).wait_recv()
        s[z * 4 + p * sp + side(o) * sq, hi] += rb3[o]
        if o == 0:
            b_q.start()

    def fin_a(h):
        part = fin.at[c, pl.ds(h * qh, qh)]
        return remote(part, part, f_s.at[0], f_r.at[0], twin)

    fin_b = remote(fin.at[c, hi], fin.at[c, hi], f_s.at[0], f_r.at[0], twin)

    def a_end(h):
        part = pl.ds(h * qh, qh)

        @pl.when(outer)
        def _():
            came(raz.at[h, 5], az_r.at[6 + h])
            fin[c, part] = s[z * 4 + here, part] + raz[h, 5]

        @pl.when(inner)
        def _():
            came(raz.at[h, pl.ds(3, 2)], az_r.at[6 + h])
            fin[c, part] = s[z * 4 + here, part] + raz[h, 3] + raz[h, 4]

        fin_a(h).start()

    @pl.loop(0, 8)
    def _(i):
        b = pair_at(i // 2, i % 2)
        columns = pl.ds(pl.multiple_of(b * block, 2 * block), 2 * block)
        both = lax.dot_general(
            hid[:, columns], gcat[...], (((0,), (0,)), ((), ())), preferred_element_type=F32
        )
        part = both[:, :E] + both[:, E:]
        for u in range(2):
            for h in range(2):
                acc[h, b + u] = part[u * block + h * half : u * block + (h + 1) * half]
        pair_send(i).start()

        @pl.when(i > 0)
        def _():
            join(i - 1)

        @pl.when(i == 4)
        def _():
            a_turn(0, 0)

        @pl.when(i == 5)
        def _():
            b_pass(0, 0)

        @pl.when(i == 6)
        def _():
            a_turn(0, 1)
            b_pass(0, 1)

    join(7)
    total = plane_total(sco_p, 4)
    sco_s[...] = total
    sco_z[z] = total
    for d in range(1, LEVELS):
        line_copy(d, sco_s, sco_z, 4).start()
    b_pass(3, 0)
    b_pass(1, 0)
    a_turn(1, 0)
    a_join(0)
    a_out(0)
    b_pass(3, 1)
    b_pass(1, 1)
    a_turn(1, 1)
    a_pass(0, 0)
    a_turn(2, 0)
    a_pass(0, 1)
    a_join(1)
    a_out(1)
    b_end()
    for o in range(2):
        b_p(o).start()
    a_p(3, 1).start()
    a_turn(2, 1)
    a_pass(1, 0)
    a_turn(3, 0)
    a_pass(1, 1)
    a_join(2)
    a_out(2)
    a_pass(3, 0)
    a_pass(3, 1)
    b_turn(0)
    b_turn(1)
    came(sco_z.at[pl.ds(0, LEVELS - 1)], st.at[7])
    mean_score = jnp.sum(sco_z[...], axis=0) / live
    bal_ref[...] = jnp.broadcast_to(jnp.sum(fraction * mean_score, axis=1, keepdims=True), bal_ref.shape)
    a_turn(3, 1)
    b_q.wait_recv()
    fin[c, hi] = s[z * 4 + here, hi] + rb3[2]
    fin_b.start()
    a_join(3)
    a_end(0)
    a_end(1)
    came(fin.at[1 - c], f_r.at[0])
    out_ref[pl.ds(0, half), :] = fin[0]
    out_ref[pl.ds(half, half), :] = fin[1]

    near = pl.ds(0, PLANE - 1)
    sent(cnt_p.at[near], st.at[0])
    sent(sco_p.at[near], st.at[4])
    sent(sco_z.at[near], st.at[6])
    for k in range(LEVELS):
        @pl.when(z == k)
        def _():
            if k < LEVELS - 1:
                sent(cnt_z.at[pl.ds(0, LEVELS - 1 - k)], st.at[2])
            if k > 0:
                sent(cnt_d.at[pl.ds(0, PLANE * k)], st.at[8])

    sent(s, d_s.at[0])
    sent(ra1, ap_s.at[0])
    sent(ra2, aq_s.at[0])
    sent(raz.at[0], az_s.at[0])
    sent(rbz.at[pl.ds(0, 3)], bz_s.at[0])
    sent(rb3, bp_s.at[0])
    sent(fin.at[c], f_s.at[0])


def store(grad, bal, grad_out, bal_out, one, sem):
    grad_copy = pltpu.make_async_copy(grad, grad_out, sem.at[0])
    grad_copy.start()
    one[0] = bal[0, 0]
    bal_copy = pltpu.make_async_copy(one, bal_out, sem.at[1])
    bal_copy.start()
    grad_copy.wait()
    bal_copy.wait()


def fused(hidden, router_weight, expert_index, lengths):
    n = lax.axis_size("ctx")
    tok, width = hidden.shape
    block = width // n
    half = block // 2
    qb = half * 3 // 14
    qa = half - qb
    dma = pltpu.SemaphoreType.DMA
    vm = pltpu.VMEM
    grad, bal = pl.pallas_call(
        functools.partial(kernel, n),
        out_shape=(pltpu.VMEM((block, E), F32), pltpu.VMEM((1, 128), F32)),
        in_specs=[
            pl.BlockSpec(memory_space=pltpu.HBM),
            pl.BlockSpec(memory_space=pltpu.HBM),
            pl.BlockSpec(memory_space=pltpu.HBM),
            pl.BlockSpec(memory_space=pltpu.HBM),
        ],
        out_specs=(pl.BlockSpec(memory_space=pltpu.VMEM), pl.BlockSpec(memory_space=pltpu.VMEM)),
        scratch_shapes=[
            pltpu.SMEM((1,), jnp.int32), vm((TOPK, tok), jnp.int32), vm((tok, width), BF16), vm((width, E), BF16),
            vm((tok, E), F32), vm((tok, E), F32), vm((tok, 2 * E), BF16),
            vm((2, n, half, E), F32), vm((n, half, E), F32), vm((2, half, E), F32),
            vm((1, E), F32), vm((PLANE, 1, E), F32), vm((1, E), F32), vm((LEVELS, 1, E), F32),
            vm((PLANE * (LEVELS - 1), 1, E), F32), vm((1, E), F32),
            vm((1, E), F32), vm((PLANE, 1, E), F32), vm((1, E), F32), vm((LEVELS, 1, E), F32),
            vm((4, 2, qa, E), F32), vm((4, qa, E), F32), vm((2, 6, qa // 2, E), F32), vm((6, 2, 2, qb, E), F32),
            vm((3, qb, E), F32), pltpu.SemaphoreType.REGULAR,
            dma((2 * CHUNKS + 2,)), dma((10,)), dma((1,)), dma((8,)),
            dma((1,)), dma((8,)), dma((1,)), dma((4,)), dma((1,)), dma((8,)), dma((1,)), dma((7,)),
            dma((1,)), dma((3,)), dma((1,)), dma((1,)),
        ],
        compiler_params=pltpu.CompilerParams(
            collective_id=0, has_side_effects=True, vmem_limit_bytes=62914560
        ),
    )(hidden, router_weight, expert_index.T, lengths)
    return pl.pallas_call(
        store,
        out_shape=(jax.ShapeDtypeStruct((block, E), F32), jax.ShapeDtypeStruct((1,), F32)),
        in_specs=[pl.BlockSpec(memory_space=pltpu.VMEM), pl.BlockSpec(memory_space=pltpu.VMEM)],
        out_specs=(pl.BlockSpec(memory_space=pltpu.HBM), pl.BlockSpec(memory_space=pltpu.HBM)),
        scratch_shapes=[pltpu.SMEM((1,), F32), dma((2,))],
        compiler_params=pltpu.CompilerParams(vmem_limit_bytes=1 << 20),
    )(grad, bal)


def solution(mesh):
    local = fused if (mesh.shape["seq"], mesh.shape["ctx"]) == (2, 16) else shards
    return jax.shard_map(
        local,
        mesh=mesh,
        in_specs=(P(("seq", "ctx"), None), P(), P(("seq", "ctx"), None), P("seq")),
        out_specs=(P("ctx", None), P("seq")),
        check_vma=False,
    )
```

```python
import functools

import jax
import jax.numpy as jnp
from jax import lax
from jax.experimental import pallas as pl
from jax.experimental.pallas import tpu as pltpu
from jax.sharding import PartitionSpec as P

E = 256
TOPK = 8


loss_scale = 65536.0


def shards(hidden, router_weight, expert_index, lengths):
    tok_rows = hidden.shape[0]
    width = hidden.shape[1]
    length_here = lengths[0]
    tokens_live = length_here.astype(jnp.float32)
    positions = lax.axis_index("ctx") * tok_rows + jnp.arange(tok_rows, dtype=jnp.int32)
    valid_mask = (positions < length_here).astype(jnp.float32)
    expert_ids = jnp.arange(E, dtype=jnp.int32)
    expert_hits = jnp.sum((expert_index[:, :, None] == expert_ids).astype(jnp.float32), axis=1)
    counts_local = jnp.sum(valid_mask[:, None] * expert_hits, axis=0)
    logits = jnp.dot(hidden, router_weight, preferred_element_type=jnp.float32)
    scores = jax.nn.sigmoid(logits)
    row_total = jnp.sum(scores, axis=1, keepdims=True)
    share_of = scores / row_total
    score_local = jnp.sum(valid_mask[:, None] * share_of, axis=0)
    counts_all, score_all = lax.psum((counts_local, score_local), "ctx")
    fraction = E * counts_all / (TOPK * tokens_live)
    mean_score = score_all / tokens_live
    balance = jnp.sum(fraction * mean_score).reshape(1)
    weights = loss_scale * fraction / tokens_live
    weighted = jnp.sum(weights * share_of, axis=1, keepdims=True)
    grad_logits = (weights - weighted) / row_total * scores * (1.0 - scores) * valid_mask[:, None]
    seq_count = lax.axis_size("seq")
    ctx_count = lax.axis_size("ctx")
    block_rows = width // (seq_count * ctx_count)
    reordered = hidden.reshape(tok_rows, ctx_count, seq_count, block_rows)
    reordered = jnp.transpose(reordered, (0, 2, 1, 3)).reshape(tok_rows, width)
    columns = reordered.astype(jnp.float32)
    block_sum = lax.psum_scatter(
        lax.dot_general(
            columns,
            grad_logits,
            (((0,), (0,)), ((), ())),
            precision=lax.Precision.HIGHEST,
            preferred_element_type=jnp.float32,
        ),
        ("seq", "ctx"),
        scatter_dimension=0,
        tiled=True,
    )
    router_grad = lax.all_gather(block_sum, "seq", axis=0, tiled=True)
    return (router_grad, balance)


MESH = pl.DeviceIdType.MESH
F32 = jnp.float32
BF16 = jnp.bfloat16
CHUNKS = 7
PARTS = 2
SMALL = 4
PLANE = 4
LEVELS = 4


def remote(src, dst, send, recv, device):
    return pltpu.make_async_remote_copy(
        src_ref=src, dst_ref=dst, send_sem=send, recv_sem=recv, device_id=device, device_id_type=MESH
    )


def kernel(
    n, hid_ref, w_ref, idx_ref, len_ref, out_ref, bal_ref,
    idx, hid, w, sh, un, gcat, acc, s, fin,
    cnt, cnt_p, cnt_s, cnt_z, cnt_d, tot, sco, sco_p, sco_s, sco_z,
    ra1, ra2, raz, rbz, rb3,
    up, in_sem, st, out_s, d_r, ap_r, aq_r, az_r, bz_r, bp_r, f_r,
):
    c = lax.axis_index("seq")
    me = lax.axis_index("ctx")
    x, y, z = me % 2, (me // 2) % 2, me // 4
    sp, sq = 1 + c, 2 - c
    p = x + c * (y - x)
    q = y + c * (x - y)
    here = p * sp + q * sq
    p_dev = (c, z * 4 + (1 - p) * sp + q * sq)
    q_dev = (c, z * 4 + p * sp + (1 - q) * sq)
    mate_z, across_z = z + 1 - 2 * (z % 2), 3 - z
    zs = [3 * (1 - z // 2), 2 - z // 2, mate_z, z]
    mate = (c, mate_z * 4 + here)
    across = (c, across_z * 4 + here)
    outer = (z == 0) | (z == 3)
    inner = (z == 1) | (z == 2)
    twin = (1 - c, me)

    def plane_peer(d):
        return (c, z * 4 + (here + d) % PLANE)

    def line_peer(d):
        return (c, ((z + d) % LEVELS) * 4 + here)

    tok, width = hid.shape
    part_w = width // CHUNKS
    big = tok // PARTS
    small = tok // SMALL
    block = width // n
    half = block // 2
    qb = half * 3 // 14
    qa = half - qb
    qh = qa // 2

    idx_copy = pltpu.make_async_copy(idx_ref, idx, in_sem.at[CHUNKS])
    idx_copy.start()

    def w_copy(i):
        span = pl.ds(pl.multiple_of(i * part_w, part_w), part_w)
        return pltpu.make_async_copy(w_ref.at[span], w.at[span], in_sem.at[i])

    def hid_copy(i):
        span = pl.ds(pl.multiple_of(i * part_w, part_w), part_w)
        return pltpu.make_async_copy(hid_ref.at[:, span], hid.at[:, span], in_sem.at[i])

    def loaded(i):
        both = hid.at[:, pl.ds(0, part_w + part_w * E // tok)]
        pltpu.make_async_copy(both, both, in_sem.at[i]).wait()

    @pl.loop(0, CHUNKS)
    def _(i):
        w_copy(i).start()
        hid_copy(i).start()

    length_here = len_ref[0]
    live = jnp.full((1, E), length_here, jnp.int32).astype(F32)

    barrier = pltpu.get_barrier_semaphore()
    for d in range(1, PLANE):
        pl.semaphore_signal(barrier, inc=1, device_id=plane_peer(d), device_id_type=MESH)
    pl.semaphore_signal(barrier, inc=1, device_id=twin, device_id_type=MESH)

    @pl.loop((z + 1) * PLANE, n)
    def _(d):
        pl.semaphore_signal(barrier, inc=1, device_id=(c, d), device_id_type=MESH)

    def count_step(i, total):
        span = pl.ds(pl.multiple_of(i * big, big), big)
        ids = lax.broadcasted_iota(jnp.int32, (E, big), 0).astype(BF16)
        named = idx[:, span].astype(F32)
        hits = jnp.zeros((E, big), BF16)
        for k in range(TOPK):
            one = jnp.broadcast_to(named[k : k + 1, :], (E, big)).astype(BF16)
            hits = hits + jnp.where(one == ids, BF16(1), BF16(0))
        at = me * tok + i * big + lax.broadcasted_iota(jnp.int32, (8, big), 1)
        valid = (at < length_here).astype(F32).astype(BF16)
        return total + lax.dot_general(
            valid, hits, (((1,), (1,)), ((), ())), preferred_element_type=F32
        )

    def plane_copy(d, src, everyone, base):
        return remote(src, everyone.at[here], st.at[base], st.at[base + 1], plane_peer(d))

    def line_copy(d, src, everyone, base):
        return remote(src, everyone.at[z], st.at[base + 2], st.at[base + 3], line_peer(d))

    def down_copy(d):
        slot = (z - d // PLANE - 1) * PLANE + here
        return remote(cnt, cnt_d.at[slot], st.at[8], st.at[9], (c, d))

    def up_copy(d):
        return remote(cnt_s, cnt_z.at[z], st.at[2], st.at[3], (c, d * PLANE + here))

    def sent(ref, sem):
        remote(ref, ref, sem, sem, twin).wait_send()

    def came(ref, sem):
        remote(ref, ref, sem, sem, twin).wait_recv()

    def plane_send(value, src, everyone, base):
        src[...] = value
        everyone[here] = value
        for d in range(1, PLANE):
            plane_copy(d, src, everyone, base).start()

    def plane_total(everyone, base):
        came(everyone.at[pl.ds(0, PLANE - 1)], st.at[base + 1])
        return jnp.sum(everyone[...], axis=0)
    idx_copy.wait()
    counts = lax.fori_loop(0, PARTS, count_step, jnp.zeros((8, E), F32))[:1]
    pl.semaphore_wait(barrier, PLANE * (z + 1))

    @pl.loop(0, z)
    def _(d):
        pl.semaphore_signal(up, inc=1, device_id=(c, d * PLANE + here), device_id_type=MESH)
    plane_send(counts, cnt, cnt_p, 0)

    @pl.loop(0, z * PLANE)
    def _(d):
        down_copy(d).start()

    sh[...] = jnp.zeros_like(sh)
    turn = 5 - (x + y + 1) // 2

    def logit_step(i):
        @pl.when(i == turn)
        def _():
            total = plane_total(cnt_p, 0)
            cnt_s[...] = total
            tot[...] = total

            @pl.when(z < LEVELS - 1)
            def _():
                pl.semaphore_wait(up, LEVELS - 1 - z)

            @pl.loop(z + 1, LEVELS)
            def _(d):
                up_copy(d).start()

        span = pl.ds(pl.multiple_of(i * part_w, part_w), part_w)
        loaded(i)
        sh[...] += jnp.dot(hid[:, span], w[span, :], preferred_element_type=F32)

    pl.loop(0, CHUNKS - 1)(logit_step)
    loaded(CHUNKS - 1)
    last = pl.ds((CHUNKS - 1) * part_w, part_w)

    def score_step(i, total):
        span = pl.ds(i * small, small)
        logits = sh[span, :] + jnp.dot(hid[span, last], w[last, :], preferred_element_type=F32)
        scores = jax.nn.sigmoid(logits)
        at = me * tok + i * small + lax.broadcasted_iota(jnp.int32, (small, 1), 0)
        valid = (at < length_here).astype(F32)
        share = scores / jnp.sum(scores, axis=1, keepdims=True)
        live_share = share * valid
        sh[span, :] = share
        un[span, :] = live_share * (1.0 - scores)
        return total + jnp.sum(live_share, axis=0, keepdims=True)

    score_local = jnp.zeros((1, E), F32)
    for i in range(SMALL):
        score_local = score_step(i, score_local)
    for k in range(LEVELS):
        @pl.when(z == k)
        def _():
            total = tot[...]
            if k < LEVELS - 1:
                far = pl.ds(0, PLANE * (LEVELS - 1 - k))
                came(cnt_d.at[far], st.at[9])
                total = total + jnp.sum(cnt_d[far], axis=0)
            if k > 0:
                near = pl.ds(0, k)
                came(cnt_z.at[near], st.at[3])
                total = total + jnp.sum(cnt_z[near], axis=0)
            tot[...] = total

    fraction = E * tot[...] / (TOPK * live)
    weights = loss_scale * fraction / live

    @pl.loop(0, PARTS)
    def _(i):
        span = pl.ds(pl.multiple_of(i * big, big), big)
        weighted = jnp.sum(weights * sh[span, :], axis=1, keepdims=True)
        grad = (weights - weighted) * un[span, :]
        top = grad.astype(BF16)
        gcat[span, :E] = top
        gcat[span, E:] = (grad - top.astype(F32)).astype(BF16)

    plane_send(score_local, sco, sco_p, 4)

    def level(k):
        return jnp.where(k == 0, zs[0], jnp.where(k == 1, zs[1], jnp.where(k == 2, zs[2], zs[3])))

    def pair_at(k, j):
        row = (1 - y) + j * (2 * y - 1)
        zk = zs[k] if isinstance(k, int) else level(k)
        return zk * 4 + 2 * row

    def pair_send(i):
        pair = pl.ds(pair_at(i // 2, i % 2), 2)
        return remote(acc.at[1 - c, pair], s.at[pair], out_s.at[0], d_r.at[i], twin)

    lo, hi = pl.ds(0, qa), pl.ds(qa, qb)

    def side(o):
        return (1 - q) + o * (2 * q - 1)

    def a_p(k, o):
        zk = zs[k] if isinstance(k, int) else level(k)
        return remote(
            s.at[zk * 4 + (1 - p) * sp + side(o) * sq, lo], ra1.at[k, o], out_s.at[0], ap_r.at[2 * k + o], p_dev
        )

    def a_q(k):
        return remote(s.at[zs[k] * 4 + p * sp + (1 - q) * sq, lo], ra2.at[k], out_s.at[0], aq_r.at[k], q_dev)

    def a_at(k, h):
        return s.at[zs[k] * 4 + here, pl.ds(h * qh, qh)]

    def b_at(k, j):
        return s.at[pl.ds(pair_at(k, j), 2), hi]

    TO = [mate, mate, mate, across, across, mate]
    OF = [0, 1, 2, 0, 1, 2]
    AT = [0, 1, 3, 2, 4, 5]

    def a_z(i, h):
        return remote(a_at(OF[i], h), raz.at[h, AT[i]], out_s.at[0], az_r.at[min(2 * AT[i], 6) + h], TO[i])

    def b_z(i, h):
        return remote(b_at(OF[i], h), rbz.at[AT[i], h], out_s.at[0], bz_r.at[2 * AT[i] + h if AT[i] < 3 else 6], TO[i])

    def b_z_out(k, j):
        pair = pl.ds(pair_at(k, j), 2)
        slot = k + k // 2
        return remote(s.at[pair, hi], rbz.at[slot, j], out_s.at[0], bz_r.at[jnp.minimum(2 * slot + j, 6)], mate)

    def join(i):
        k, j = i // 2, i % 2
        pair_send(i).wait_recv()
        pair = pl.ds(pair_at(k, j), 2)
        s[pair] += acc[c, pair]

        early = (k < 3) | (inner & (i == 6))

        @pl.when((c == 0) & early)
        def _():
            a_p(k, j).start()

        @pl.when((c == 1) & (j == 0) & early)
        def _():
            a_p(k, 0).start()

        @pl.when((c == 1) & (j == 0) & (k < 3))
        def _():
            a_p(k, 1).start()

        @pl.when(outer & (k < 3))
        def _():
            b_z_out(k, j).start()

    def a_turn(k, o):
        a_p(k, o).wait_recv()
        s[zs[k] * 4 + p * sp + side(o) * sq, lo] += ra1[k, o]
        if o == 0:
            a_q(k).start()

    def a_join(k):
        a_q(k).wait_recv()
        s[zs[k] * 4 + here, lo] += ra2[k]

    def a_out(k):
        @pl.when(outer)
        def _():
            for h in range(2):
                a_z(k, h).start()

    def passing(copies, at, got, slot, k, out, h):
        copies(slot, h).wait_recv()
        at(k, h)[...] += got[h, AT[slot]] if got is raz else got[AT[slot], h]
        copies(out, h).start()

    def b_pass(slot, h):
        k, out = {0: (0, 3), 1: (1, 4), 3: (2, 5)}[slot]

        @pl.when(inner)
        def _():
            passing(b_z, b_at, rbz, slot, k, out, h)

    def a_pass(slot, h):
        k, out = {0: (0, 3), 1: (1, 4), 3: (2, 5)}[slot]

        @pl.when(inner)
        def _():
            passing(a_z, a_at, raz, slot, k, out, h)

    def b_end():
        @pl.when(outer)
        def _():
            came(rbz.at[5], bz_r.at[6])
            for h in range(2):
                b_at(3, h)[...] += rbz[5, h]

        @pl.when(inner)
        def _():
            came(rbz.at[pl.ds(3, 2)], bz_r.at[6])
            for h in range(2):
                b_at(3, h)[...] += rbz[3, h] + rbz[4, h]

    def b_p(o):
        return remote(s.at[z * 4 + (1 - p) * sp + side(o) * sq, hi], rb3.at[o], out_s.at[0], bp_r.at[o], p_dev)

    b_q = remote(s.at[z * 4 + p * sp + (1 - q) * sq, hi], rb3.at[2], out_s.at[0], bp_r.at[2], q_dev)

    def b_turn(o):
        b_p(o).wait_recv()
        s[z * 4 + p * sp + side(o) * sq, hi] += rb3[o]
        if o == 0:
            b_q.start()

    def fin_a(h):
        part = fin.at[c, pl.ds(h * qh, qh)]
        return remote(part, part, out_s.at[0], f_r.at[0], twin)

    fin_b = remote(fin.at[c, hi], fin.at[c, hi], out_s.at[0], f_r.at[0], twin)

    def a_end(h):
        part = pl.ds(h * qh, qh)

        @pl.when(outer)
        def _():
            came(raz.at[h, 5], az_r.at[6 + h])
            fin[c, part] = s[z * 4 + here, part] + raz[h, 5]

        @pl.when(inner)
        def _():
            came(raz.at[h, pl.ds(3, 2)], az_r.at[6 + h])
            fin[c, part] = s[z * 4 + here, part] + raz[h, 3] + raz[h, 4]

        fin_a(h).start()

    @pl.loop(0, 8)
    def _(i):
        b = pair_at(i // 2, i % 2)
        columns = pl.ds(pl.multiple_of(b * block, 2 * block), 2 * block)
        both = lax.dot_general(
            hid[:, columns], gcat[...], (((0,), (0,)), ((), ())), preferred_element_type=F32
        )
        part = both[:, :E] + both[:, E:]
        for u in range(2):
            for h in range(2):
                acc[h, b + u] = part[u * block + h * half : u * block + (h + 1) * half]
        pair_send(i).start()

        @pl.when(i > 0)
        def _():
            join(i - 1)

        @pl.when(i == 4)
        def _():
            a_turn(0, 0)

        @pl.when(i == 5)
        def _():
            b_pass(0, 0)

        @pl.when(i == 6)
        def _():
            a_turn(0, 1)
            b_pass(0, 1)

    join(7)
    total = plane_total(sco_p, 4)
    sco_s[...] = total
    sco_z[z] = total
    for d in range(1, LEVELS):
        line_copy(d, sco_s, sco_z, 4).start()
    b_pass(3, 0)
    b_pass(1, 0)
    a_turn(1, 0)
    a_join(0)
    a_out(0)
    b_pass(3, 1)
    b_pass(1, 1)
    a_turn(1, 1)
    a_turn(2, 0)
    a_pass(0, 0)
    a_pass(0, 1)
    a_join(1)
    a_out(1)
    @pl.when(outer)
    def _():
        a_p(3, 0).start()
    b_end()
    for o in range(2):
        b_p(o).start()

    @pl.when(outer)
    def _():
        a_turn(2, 1)
        a_p(3, 1).start()
        a_join(2)
        a_out(2)
        a_turn(3, 0)
        b_turn(0)
        b_turn(1)

    @pl.when(inner)
    def _():
        a_p(3, 1).start()
        a_turn(2, 1)
        a_pass(1, 0)
        a_turn(3, 0)
        a_pass(1, 1)
        a_join(2)
        a_pass(3, 0)
        a_pass(3, 1)
        b_turn(0)
        b_turn(1)
    came(sco_z.at[pl.ds(0, LEVELS - 1)], st.at[7])
    mean_score = jnp.sum(sco_z[...], axis=0) / live
    bal_ref[...] = jnp.broadcast_to(jnp.sum(fraction * mean_score, axis=1, keepdims=True), bal_ref.shape)
    a_turn(3, 1)
    b_q.wait_recv()
    fin[c, hi] = s[z * 4 + here, hi] + rb3[2]
    fin_b.start()
    a_join(3)
    a_end(0)
    a_end(1)
    came(fin.at[1 - c], f_r.at[0])
    out_ref[pl.ds(0, half), :] = fin[0]
    out_ref[pl.ds(half, half), :] = fin[1]

    near = pl.ds(0, PLANE - 1)
    sent(cnt_p.at[near], st.at[0])
    sent(sco_p.at[near], st.at[4])
    sent(sco_z.at[near], st.at[6])
    for k in range(LEVELS):
        @pl.when(z == k)
        def _():
            if k < LEVELS - 1:
                sent(cnt_z.at[pl.ds(0, LEVELS - 1 - k)], st.at[2])
            if k > 0:
                sent(cnt_d.at[pl.ds(0, PLANE * k)], st.at[8])

    sent(acc, out_s.at[0])


def store(grad, bal, grad_out, bal_out, one, sem):
    rows = grad.shape[0] // 4
    spans = [pl.ds(i * rows, rows) for i in range(4)]
    copies = [pltpu.make_async_copy(grad.at[span], grad_out.at[span], sem.at[i]) for i, span in enumerate(spans)]
    for copy in copies:
        copy.start()
    one[0] = bal[0, 0]
    bal_copy = pltpu.make_async_copy(one, bal_out, sem.at[4])
    bal_copy.start()
    for copy in copies:
        copy.wait()
    bal_copy.wait()


def fused(hidden, router_weight, expert_index, lengths):
    n = lax.axis_size("ctx")
    tok, width = hidden.shape
    block = width // n
    half = block // 2
    qb = half * 3 // 14
    qa = half - qb
    dma = pltpu.SemaphoreType.DMA
    vm = pltpu.VMEM
    grad, bal = pl.pallas_call(
        functools.partial(kernel, n),
        out_shape=(pltpu.VMEM((block, E), F32), pltpu.VMEM((1, 128), F32)),
        in_specs=[
            pl.BlockSpec(memory_space=pltpu.HBM),
            pl.BlockSpec(memory_space=pltpu.HBM),
            pl.BlockSpec(memory_space=pltpu.HBM),
            pl.BlockSpec(memory_space=pltpu.SMEM),
        ],
        out_specs=(pl.BlockSpec(memory_space=pltpu.VMEM), pl.BlockSpec(memory_space=pltpu.VMEM)),
        scratch_shapes=[
            vm((TOPK, tok), jnp.int32), vm((tok, width), BF16), vm((width, E), BF16),
            vm((tok, E), F32), vm((tok, E), F32), vm((tok, 2 * E), BF16),
            vm((2, n, half, E), F32), vm((n, half, E), F32), vm((2, half, E), F32),
            vm((1, E), F32), vm((PLANE, 1, E), F32), vm((1, E), F32), vm((LEVELS, 1, E), F32),
            vm((PLANE * (LEVELS - 1), 1, E), F32), vm((1, E), F32),
            vm((1, E), F32), vm((PLANE, 1, E), F32), vm((1, E), F32), vm((LEVELS, 1, E), F32),
            vm((4, 2, qa, E), F32), vm((4, qa, E), F32), vm((2, 6, qa // 2, E), F32), vm((6, 2, 2, qb, E), F32),
            vm((3, qb, E), F32), pltpu.SemaphoreType.REGULAR,
            dma((CHUNKS + 1,)), dma((10,)), dma((1,)), dma((8,)),
            dma((8,)), dma((4,)), dma((8,)), dma((7,)), dma((3,)), dma((1,)),
        ],
        compiler_params=pltpu.CompilerParams(
            collective_id=0, has_side_effects=True, vmem_limit_bytes=62914560
        ),
    )(hidden, router_weight, expert_index.T, lengths)
    return pl.pallas_call(
        store,
        out_shape=(jax.ShapeDtypeStruct((block, E), F32), jax.ShapeDtypeStruct((1,), F32)),
        in_specs=[pl.BlockSpec(memory_space=pltpu.VMEM), pl.BlockSpec(memory_space=pltpu.VMEM)],
        out_specs=(pl.BlockSpec(memory_space=pltpu.HBM), pl.BlockSpec(memory_space=pltpu.HBM)),
        scratch_shapes=[pltpu.SMEM((1,), F32), dma((5,))],
        compiler_params=pltpu.CompilerParams(vmem_limit_bytes=1 << 20),
    )(grad, bal)


def solution(mesh):
    local = fused if (mesh.shape["seq"], mesh.shape["ctx"]) == (2, 16) else shards
    return jax.shard_map(
        local,
        mesh=mesh,
        in_specs=(P(("seq", "ctx"), None), P(), P(("seq", "ctx"), None), P("seq")),
        out_specs=(P("ctx", None), P("seq")),
        check_vma=False,
    )
```

```python
import functools

import jax
import jax.numpy as jnp
from jax import lax
from jax.experimental import pallas as pl
from jax.experimental.pallas import tpu as pltpu
from jax.sharding import PartitionSpec as P

E = 256
TOPK = 8


loss_scale = 65536.0


def shards(hidden, router_weight, expert_index, lengths):
    tok_rows = hidden.shape[0]
    width = hidden.shape[1]
    length_here = lengths[0]
    tokens_live = length_here.astype(jnp.float32)
    positions = lax.axis_index("ctx") * tok_rows + jnp.arange(tok_rows, dtype=jnp.int32)
    valid_mask = (positions < length_here).astype(jnp.float32)
    expert_ids = jnp.arange(E, dtype=jnp.int32)
    expert_hits = jnp.sum((expert_index[:, :, None] == expert_ids).astype(jnp.float32), axis=1)
    counts_local = jnp.sum(valid_mask[:, None] * expert_hits, axis=0)
    logits = jnp.dot(hidden, router_weight, preferred_element_type=jnp.float32)
    scores = jax.nn.sigmoid(logits)
    row_total = jnp.sum(scores, axis=1, keepdims=True)
    share_of = scores / row_total
    score_local = jnp.sum(valid_mask[:, None] * share_of, axis=0)
    counts_all, score_all = lax.psum((counts_local, score_local), "ctx")
    fraction = E * counts_all / (TOPK * tokens_live)
    mean_score = score_all / tokens_live
    balance = jnp.sum(fraction * mean_score).reshape(1)
    weights = loss_scale * fraction / tokens_live
    weighted = jnp.sum(weights * share_of, axis=1, keepdims=True)
    grad_logits = (weights - weighted) / row_total * scores * (1.0 - scores) * valid_mask[:, None]
    seq_count = lax.axis_size("seq")
    ctx_count = lax.axis_size("ctx")
    block_rows = width // (seq_count * ctx_count)
    reordered = hidden.reshape(tok_rows, ctx_count, seq_count, block_rows)
    reordered = jnp.transpose(reordered, (0, 2, 1, 3)).reshape(tok_rows, width)
    columns = reordered.astype(jnp.float32)
    block_sum = lax.psum_scatter(
        lax.dot_general(
            columns,
            grad_logits,
            (((0,), (0,)), ((), ())),
            precision=lax.Precision.HIGHEST,
            preferred_element_type=jnp.float32,
        ),
        ("seq", "ctx"),
        scatter_dimension=0,
        tiled=True,
    )
    router_grad = lax.all_gather(block_sum, "seq", axis=0, tiled=True)
    return (router_grad, balance)


MESH = pl.DeviceIdType.MESH
F32 = jnp.float32
BF16 = jnp.bfloat16
CHUNKS = 7
PARTS = 2
SMALL = 4
PLANE = 4
LEVELS = 4


def remote(src, dst, send, recv, device):
    return pltpu.make_async_remote_copy(
        src_ref=src, dst_ref=dst, send_sem=send, recv_sem=recv, device_id=device, device_id_type=MESH
    )


def kernel(
    n, hid_ref, w_ref, idx_ref, len_ref, out_ref, bal_ref,
    idx, hid, w, sh, un, gcat, acc, s, fin,
    cnt, cnt_p, cnt_s, cnt_z, cnt_d, tot, sco, sco_p, sco_s, sco_z,
    ra1, ra2, raz, rbz, rb3,
    up, in_sem, st, out_s, d_r, ap_r, aq_r, az_r, bz_r, bp_r, f_r,
):
    c = lax.axis_index("seq")
    me = lax.axis_index("ctx")
    x, y, z = me % 2, (me // 2) % 2, me // 4
    sp, sq = 1 + c, 2 - c
    p = x + c * (y - x)
    q = y + c * (x - y)
    here = p * sp + q * sq
    p_dev = (c, z * 4 + (1 - p) * sp + q * sq)
    q_dev = (c, z * 4 + p * sp + (1 - q) * sq)
    mate_z, across_z = z + 1 - 2 * (z % 2), 3 - z
    zs = [3 * (1 - z // 2), 2 - z // 2, mate_z, z]
    mate = (c, mate_z * 4 + here)
    across = (c, across_z * 4 + here)
    outer = (z == 0) | (z == 3)
    inner = (z == 1) | (z == 2)
    twin = (1 - c, me)

    def plane_peer(d):
        return (c, z * 4 + (here + d) % PLANE)

    def line_peer(d):
        return (c, ((z + d) % LEVELS) * 4 + here)

    tok, width = hid.shape
    part_w = width // CHUNKS
    big = tok // PARTS
    small = tok // SMALL
    block = width // n
    half = block // 2
    qb = half * 3 // 14
    qa = half - qb
    qh = qa // 2

    idx_copy = pltpu.make_async_copy(idx_ref, idx, in_sem.at[CHUNKS])
    idx_copy.start()

    def w_copy(i):
        span = pl.ds(pl.multiple_of(i * part_w, part_w), part_w)
        return pltpu.make_async_copy(w_ref.at[span], w.at[span], in_sem.at[i])

    def hid_copy(i):
        span = pl.ds(pl.multiple_of(i * part_w, part_w), part_w)
        return pltpu.make_async_copy(hid_ref.at[:, span], hid.at[:, span], in_sem.at[i])

    def loaded(i):
        both = hid.at[:, pl.ds(0, part_w + part_w * E // tok)]
        pltpu.make_async_copy(both, both, in_sem.at[i]).wait()

    @pl.loop(0, CHUNKS)
    def _(i):
        w_copy(i).start()
        hid_copy(i).start()

    length_here = len_ref[0]
    live = jnp.full((1, E), length_here, jnp.int32).astype(F32)

    barrier = pltpu.get_barrier_semaphore()
    for d in range(1, PLANE):
        pl.semaphore_signal(barrier, inc=1, device_id=plane_peer(d), device_id_type=MESH)
    pl.semaphore_signal(barrier, inc=1, device_id=twin, device_id_type=MESH)

    @pl.loop((z + 1) * PLANE, n)
    def _(d):
        pl.semaphore_signal(barrier, inc=1, device_id=(c, d), device_id_type=MESH)

    def count_step(i, total):
        span = pl.ds(pl.multiple_of(i * big, big), big)
        ids = lax.broadcasted_iota(jnp.int32, (E, big), 0).astype(BF16)
        named = idx[:, span].astype(F32)
        hits = jnp.zeros((E, big), BF16)
        for k in range(TOPK):
            one = jnp.broadcast_to(named[k : k + 1, :], (E, big)).astype(BF16)
            hits = hits + jnp.where(one == ids, BF16(1), BF16(0))
        at = me * tok + i * big + lax.broadcasted_iota(jnp.int32, (8, big), 1)
        valid = (at < length_here).astype(F32).astype(BF16)
        return total + lax.dot_general(
            valid, hits, (((1,), (1,)), ((), ())), preferred_element_type=F32
        )

    def plane_copy(d, src, everyone, base):
        return remote(src, everyone.at[here], st.at[base], st.at[base + 1], plane_peer(d))

    def line_copy(d, src, everyone, base):
        return remote(src, everyone.at[z], st.at[base + 2], st.at[base + 3], line_peer(d))

    def down_copy(d):
        slot = (z - d // PLANE - 1) * PLANE + here
        return remote(cnt, cnt_d.at[slot], st.at[8], st.at[9], (c, d))

    def up_copy(d):
        return remote(cnt_s, cnt_z.at[z], st.at[2], st.at[3], (c, d * PLANE + here))

    def sent(ref, sem):
        remote(ref, ref, sem, sem, twin).wait_send()

    def came(ref, sem):
        remote(ref, ref, sem, sem, twin).wait_recv()

    def plane_send(value, src, everyone, base):
        src[...] = value
        everyone[here] = value
        for d in range(1, PLANE):
            plane_copy(d, src, everyone, base).start()

    def plane_total(everyone, base):
        came(everyone.at[pl.ds(0, PLANE - 1)], st.at[base + 1])
        return jnp.sum(everyone[...], axis=0)
    idx_copy.wait()
    counts = lax.fori_loop(0, PARTS, count_step, jnp.zeros((8, E), F32))[:1]
    pl.semaphore_wait(barrier, PLANE * (z + 1))

    @pl.loop(0, z)
    def _(d):
        pl.semaphore_signal(up, inc=1, device_id=(c, d * PLANE + here), device_id_type=MESH)
    plane_send(counts, cnt, cnt_p, 0)

    @pl.loop(0, z * PLANE)
    def _(d):
        down_copy(d).start()

    sh[...] = jnp.zeros_like(sh)
    turn = 5 - (x + y + 1) // 2

    def logit_step(i):
        @pl.when(i == turn)
        def _():
            total = plane_total(cnt_p, 0)
            cnt_s[...] = total
            tot[...] = total

            @pl.when(z < LEVELS - 1)
            def _():
                pl.semaphore_wait(up, LEVELS - 1 - z)

            @pl.loop(z + 1, LEVELS)
            def _(d):
                up_copy(d).start()

        span = pl.ds(pl.multiple_of(i * part_w, part_w), part_w)
        loaded(i)
        sh[...] += jnp.dot(hid[:, span], w[span, :], preferred_element_type=F32)

    pl.loop(0, CHUNKS - 1)(logit_step)
    loaded(CHUNKS - 1)
    last = pl.ds((CHUNKS - 1) * part_w, part_w)

    def score_step(i, total):
        span = pl.ds(i * small, small)
        logits = sh[span, :] + jnp.dot(hid[span, last], w[last, :], preferred_element_type=F32)
        scores = jax.nn.sigmoid(logits)
        at = me * tok + i * small + lax.broadcasted_iota(jnp.int32, (small, 1), 0)
        valid = (at < length_here).astype(F32)
        share = scores / jnp.sum(scores, axis=1, keepdims=True)
        live_share = share * valid
        sh[span, :] = share
        un[span, :] = live_share * (1.0 - scores)
        return total + jnp.sum(live_share, axis=0, keepdims=True)

    score_local = jnp.zeros((1, E), F32)
    for i in range(SMALL):
        score_local = score_step(i, score_local)
    for k in range(LEVELS):
        @pl.when(z == k)
        def _():
            total = tot[...]
            if k < LEVELS - 1:
                far = pl.ds(0, PLANE * (LEVELS - 1 - k))
                came(cnt_d.at[far], st.at[9])
                total = total + jnp.sum(cnt_d[far], axis=0)
            if k > 0:
                near = pl.ds(0, k)
                came(cnt_z.at[near], st.at[3])
                total = total + jnp.sum(cnt_z[near], axis=0)
            tot[...] = total

    fraction = E * tot[...] / (TOPK * live)
    weights = loss_scale * fraction / live

    @pl.loop(0, PARTS)
    def _(i):
        span = pl.ds(pl.multiple_of(i * big, big), big)
        weighted = jnp.sum(weights * sh[span, :], axis=1, keepdims=True)
        grad = (weights - weighted) * un[span, :]
        top = grad.astype(BF16)
        gcat[span, :E] = top
        gcat[span, E:] = (grad - top.astype(F32)).astype(BF16)

    plane_send(score_local, sco, sco_p, 4)

    def level(k):
        return jnp.where(k == 0, zs[0], jnp.where(k == 1, zs[1], jnp.where(k == 2, zs[2], zs[3])))

    def pair_at(k, j):
        row = (1 - y) + j * (2 * y - 1)
        zk = zs[k] if isinstance(k, int) else level(k)
        return zk * 4 + 2 * row

    def pair_send(i):
        pair = pl.ds(pair_at(i // 2, i % 2), 2)
        return remote(acc.at[1 - c, pair], s.at[pair], out_s.at[0], d_r.at[i], twin)

    lo, hi = pl.ds(0, qa), pl.ds(qa, qb)

    def side(o):
        return (1 - q) + o * (2 * q - 1)

    def a_p(k, o):
        zk = zs[k] if isinstance(k, int) else level(k)
        return remote(
            s.at[zk * 4 + (1 - p) * sp + side(o) * sq, lo], ra1.at[k, o], out_s.at[0], ap_r.at[2 * k + o], p_dev
        )

    def a_q(k):
        return remote(s.at[zs[k] * 4 + p * sp + (1 - q) * sq, lo], ra2.at[k], out_s.at[0], aq_r.at[k], q_dev)

    def a_at(k, h):
        return s.at[zs[k] * 4 + here, pl.ds(h * qh, qh)]

    def b_at(k, j):
        return s.at[pl.ds(pair_at(k, j), 2), hi]

    TO = [mate, mate, mate, across, across, mate]
    OF = [0, 1, 2, 0, 1, 2]
    AT = [0, 1, 3, 2, 4, 5]

    def a_z(i, h):
        return remote(a_at(OF[i], h), raz.at[h, AT[i]], out_s.at[0], az_r.at[min(2 * AT[i], 6) + h], TO[i])

    def b_z(i, h):
        return remote(b_at(OF[i], h), rbz.at[AT[i], h], out_s.at[0], bz_r.at[2 * AT[i] + h if AT[i] < 3 else 6], TO[i])

    def b_z_out(k, j):
        pair = pl.ds(pair_at(k, j), 2)
        slot = k + k // 2
        return remote(s.at[pair, hi], rbz.at[slot, j], out_s.at[0], bz_r.at[jnp.minimum(2 * slot + j, 6)], mate)

    def join(i):
        k, j = i // 2, i % 2
        pair_send(i).wait_recv()
        pair = pl.ds(pair_at(k, j), 2)
        s[pair] += acc[c, pair]

        early = (k < 3) | (inner & (i == 6))

        @pl.when((c == 0) & early)
        def _():
            a_p(k, j).start()

        @pl.when((c == 1) & (j == 0) & early)
        def _():
            a_p(k, 0).start()

        @pl.when((c == 1) & (j == 0) & (k < 3))
        def _():
            a_p(k, 1).start()

        @pl.when(outer & (k < 3))
        def _():
            b_z_out(k, j).start()

    def a_turn(k, o):
        a_p(k, o).wait_recv()
        s[zs[k] * 4 + p * sp + side(o) * sq, lo] += ra1[k, o]
        if o == 0:
            a_q(k).start()

    def a_join(k):
        a_q(k).wait_recv()
        s[zs[k] * 4 + here, lo] += ra2[k]

    def a_out(k):
        @pl.when(outer)
        def _():
            for h in range(2):
                a_z(k, h).start()

    def passing(copies, at, got, slot, k, out, h):
        copies(slot, h).wait_recv()
        at(k, h)[...] += got[h, AT[slot]] if got is raz else got[AT[slot], h]
        copies(out, h).start()

    def b_pass(slot, h):
        k, out = {0: (0, 3), 1: (1, 4), 3: (2, 5)}[slot]

        @pl.when(inner)
        def _():
            passing(b_z, b_at, rbz, slot, k, out, h)

    def a_pass(slot, h):
        k, out = {0: (0, 3), 1: (1, 4), 3: (2, 5)}[slot]

        @pl.when(inner)
        def _():
            passing(a_z, a_at, raz, slot, k, out, h)

    def b_end():
        @pl.when(outer)
        def _():
            came(rbz.at[5], bz_r.at[6])
            for h in range(2):
                b_at(3, h)[...] += rbz[5, h]

        @pl.when(inner)
        def _():
            came(rbz.at[pl.ds(3, 2)], bz_r.at[6])
            for h in range(2):
                b_at(3, h)[...] += rbz[3, h] + rbz[4, h]

    def b_p(o):
        return remote(s.at[z * 4 + (1 - p) * sp + side(o) * sq, hi], rb3.at[o], out_s.at[0], bp_r.at[o], p_dev)

    b_q = remote(s.at[z * 4 + p * sp + (1 - q) * sq, hi], rb3.at[2], out_s.at[0], bp_r.at[2], q_dev)

    def b_turn(o):
        b_p(o).wait_recv()
        s[z * 4 + p * sp + side(o) * sq, hi] += rb3[o]
        if o == 0:
            b_q.start()

    def fin_a(h):
        part = fin.at[c, pl.ds(h * qh, qh)]
        return remote(part, part, out_s.at[0], f_r.at[0], twin)

    fin_b = remote(fin.at[c, hi], fin.at[c, hi], out_s.at[0], f_r.at[0], twin)

    def a_end(h):
        part = pl.ds(h * qh, qh)

        @pl.when(outer)
        def _():
            came(raz.at[h, 5], az_r.at[6 + h])
            fin[c, part] = s[z * 4 + here, part] + raz[h, 5]

        @pl.when(inner)
        def _():
            came(raz.at[h, pl.ds(3, 2)], az_r.at[6 + h])
            fin[c, part] = s[z * 4 + here, part] + raz[h, 3] + raz[h, 4]

        fin_a(h).start()

    @pl.loop(0, 8)
    def _(i):
        b = pair_at(i // 2, i % 2)
        columns = pl.ds(pl.multiple_of(b * block, 2 * block), 2 * block)
        both = lax.dot_general(
            hid[:, columns], gcat[...], (((0,), (0,)), ((), ())), preferred_element_type=F32
        )
        part = both[:, :E] + both[:, E:]
        for u in range(2):
            for h in range(2):
                acc[h, b + u] = part[u * block + h * half : u * block + (h + 1) * half]
        pair_send(i).start()

        @pl.when(i > 0)
        def _():
            join(i - 1)

        @pl.when(i == 4)
        def _():
            a_turn(0, 0)

        @pl.when(i == 5)
        def _():
            b_pass(0, 0)

        @pl.when(i == 6)
        def _():
            a_turn(0, 1)
            b_pass(0, 1)

    join(7)
    total = plane_total(sco_p, 4)
    sco_s[...] = total
    sco_z[z] = total
    for d in range(1, LEVELS):
        line_copy(d, sco_s, sco_z, 4).start()
    b_pass(3, 0)
    b_pass(1, 0)
    a_turn(1, 0)
    a_join(0)
    a_out(0)
    b_pass(3, 1)
    b_pass(1, 1)
    a_turn(1, 1)
    a_turn(2, 0)
    a_pass(0, 0)
    a_pass(0, 1)
    a_join(1)
    a_out(1)
    b_end()
    for o in range(2):
        b_p(o).start()

    @pl.when(outer)
    def _():
        a_turn(2, 1)
        a_p(3, 0).start()
        a_p(3, 1).start()
        a_join(2)
        a_out(2)
        b_turn(0)
        b_turn(1)
        a_turn(3, 0)

    @pl.when(inner)
    def _():
        a_p(3, 1).start()
        a_turn(2, 1)
        a_pass(1, 0)
        a_turn(3, 0)
        a_pass(1, 1)
        a_join(2)
        a_pass(3, 0)
        a_pass(3, 1)
        b_turn(0)
        b_turn(1)
    came(sco_z.at[pl.ds(0, LEVELS - 1)], st.at[7])
    mean_score = jnp.sum(sco_z[...], axis=0) / live
    bal_ref[...] = jnp.broadcast_to(jnp.sum(fraction * mean_score, axis=1, keepdims=True), bal_ref.shape)
    b_q.wait_recv()
    fin[c, hi] = s[z * 4 + here, hi] + rb3[2]
    fin_b.start()
    a_turn(3, 1)
    a_join(3)
    a_end(0)
    a_end(1)
    came(fin.at[1 - c], f_r.at[0])
    out_ref[pl.ds(0, half), :] = fin[0]
    out_ref[pl.ds(half, half), :] = fin[1]

    near = pl.ds(0, PLANE - 1)
    sent(cnt_p.at[near], st.at[0])
    sent(sco_p.at[near], st.at[4])
    sent(sco_z.at[near], st.at[6])
    for k in range(LEVELS):
        @pl.when(z == k)
        def _():
            if k < LEVELS - 1:
                sent(cnt_z.at[pl.ds(0, LEVELS - 1 - k)], st.at[2])
            if k > 0:
                sent(cnt_d.at[pl.ds(0, PLANE * k)], st.at[8])

    sent(acc, out_s.at[0])


def store(grad, bal, grad_out, bal_out, one, sem):
    rows = grad.shape[0] // 4
    spans = [pl.ds(i * rows, rows) for i in range(4)]
    copies = [pltpu.make_async_copy(grad.at[span], grad_out.at[span], sem.at[i]) for i, span in enumerate(spans)]
    for copy in copies:
        copy.start()
    one[0] = bal[0, 0]
    bal_copy = pltpu.make_async_copy(one, bal_out, sem.at[4])
    bal_copy.start()
    for copy in copies:
        copy.wait()
    bal_copy.wait()


def fused(hidden, router_weight, expert_index, lengths):
    n = lax.axis_size("ctx")
    tok, width = hidden.shape
    block = width // n
    half = block // 2
    qb = half * 3 // 14
    qa = half - qb
    dma = pltpu.SemaphoreType.DMA
    vm = pltpu.VMEM
    grad, bal = pl.pallas_call(
        functools.partial(kernel, n),
        out_shape=(pltpu.VMEM((block, E), F32), pltpu.VMEM((1, 128), F32)),
        in_specs=[
            pl.BlockSpec(memory_space=pltpu.HBM),
            pl.BlockSpec(memory_space=pltpu.HBM),
            pl.BlockSpec(memory_space=pltpu.HBM),
            pl.BlockSpec(memory_space=pltpu.SMEM),
        ],
        out_specs=(pl.BlockSpec(memory_space=pltpu.VMEM), pl.BlockSpec(memory_space=pltpu.VMEM)),
        scratch_shapes=[
            vm((TOPK, tok), jnp.int32), vm((tok, width), BF16), vm((width, E), BF16),
            vm((tok, E), F32), vm((tok, E), F32), vm((tok, 2 * E), BF16),
            vm((2, n, half, E), F32), vm((n, half, E), F32), vm((2, half, E), F32),
            vm((1, E), F32), vm((PLANE, 1, E), F32), vm((1, E), F32), vm((LEVELS, 1, E), F32),
            vm((PLANE * (LEVELS - 1), 1, E), F32), vm((1, E), F32),
            vm((1, E), F32), vm((PLANE, 1, E), F32), vm((1, E), F32), vm((LEVELS, 1, E), F32),
            vm((4, 2, qa, E), F32), vm((4, qa, E), F32), vm((2, 6, qa // 2, E), F32), vm((6, 2, 2, qb, E), F32),
            vm((3, qb, E), F32), pltpu.SemaphoreType.REGULAR,
            dma((CHUNKS + 1,)), dma((10,)), dma((1,)), dma((8,)),
            dma((8,)), dma((4,)), dma((8,)), dma((7,)), dma((3,)), dma((1,)),
        ],
        compiler_params=pltpu.CompilerParams(
            collective_id=0, has_side_effects=True, vmem_limit_bytes=62914560
        ),
    )(hidden, router_weight, expert_index.T, lengths)
    return pl.pallas_call(
        store,
        out_shape=(jax.ShapeDtypeStruct((block, E), F32), jax.ShapeDtypeStruct((1,), F32)),
        in_specs=[pl.BlockSpec(memory_space=pltpu.VMEM), pl.BlockSpec(memory_space=pltpu.VMEM)],
        out_specs=(pl.BlockSpec(memory_space=pltpu.HBM), pl.BlockSpec(memory_space=pltpu.HBM)),
        scratch_shapes=[pltpu.SMEM((1,), F32), dma((5,))],
        compiler_params=pltpu.CompilerParams(vmem_limit_bytes=1 << 20),
    )(grad, bal)


def solution(mesh):
    local = fused if (mesh.shape["seq"], mesh.shape["ctx"]) == (2, 16) else shards
    return jax.shard_map(
        local,
        mesh=mesh,
        in_specs=(P(("seq", "ctx"), None), P(), P(("seq", "ctx"), None), P("seq")),
        out_specs=(P("ctx", None), P("seq")),
        check_vma=False,
    )
```
